8 devices in a mesh: dp: 8 (over z, y, x, core).
Axes of the slice: x: 2, y: 2, z: 1, core: 2. Of those that a mesh axis runs over, the one named last changes fastest.
Arguments:
- grad_wq: bfloat16 [8, 2, 1152, 1152], P('dp')
- grad_wk: bfloat16 [8, 2, 1152, 384], P('dp')
- grad_wv: bfloat16 [8, 2, 1152, 384], P('dp')
- grad_wo: bfloat16 [8, 2, 1152, 1152], P('dp')
- grad_gate: bfloat16 [8, 2, 1152, 3072], P('dp')
- grad_up: bfloat16 [8, 2, 1152, 3072], P('dp')
- grad_down: bfloat16 [8, 2, 3072, 1152], P('dp')
- grad_attn_norm: bfloat16 [8, 2, 1152], P('dp')
- grad_mlp_norm: bfloat16 [8, 2, 1152], P('dp')
- grad_final_norm: bfloat16 [8, 1152], P('dp')
- master: float32 [28317696], P('dp')
- exp_avg: float32 [28317696], P('dp')
- exp_avg_sq: float32 [28317696], P('dp')
- learn_rate: float32 [], replicated
Outputs:
- output 1: float32 [28317696], P('dp')
- output 2: float32 [28317696], P('dp')
- output 3: float32 [28317696], P('dp')
- output 4: bfloat16 [2, 1152, 1152], replicated
- output 5: bfloat16 [2, 1152, 384], replicated
- output 6: bfloat16 [2, 1152, 384], replicated
- output 7: bfloat16 [2, 1152, 1152], replicated
- output 8: bfloat16 [2, 1152, 3072], replicated
- output 9: bfloat16 [2, 1152, 3072], replicated
- output 10: bfloat16 [2, 3072, 1152], replicated
- output 11: bfloat16 [2, 1152], replicated
- output 12: bfloat16 [2, 1152], replicated
- output 13: bfloat16 [1152], replicated
- output 14: float32 [], replicated
All inputs are finite; a program needn't handle non-finite values.
Results may differ from the reference program's by a relative error of at most 0.001.
Values sent between devices are 32-bit elements.
A program may use at most 1 GiB of HBM per device.

```python
import math
import jax
import jax.numpy as jnp

DP = 8
LAYERS = 2
D = 1152
HEADS = 18
KV_HEADS = 6
HEAD = 64
FF = 3072
STEP = 4

Q_DIM = HEADS * HEAD
KV_DIM = KV_HEADS * HEAD
MATRIX_COUNT = LAYERS * (2 * D * Q_DIM + 2 * D * KV_DIM + 3 * D * FF)
TOTAL = MATRIX_COUNT + 2 * LAYERS * D + D
PADDED = -(-TOTAL // (DP * 128)) * DP * 128
BETA_ONE = 0.9
BETA_TWO = 0.95
ADAM_EPS = 1e-8
WEIGHT_DECAY = 0.1
MAX_NORM = 1.0
CLIP_EPS = 1e-6
BIAS_ONE = 1.0 - BETA_ONE ** STEP
BIAS_TWO = 1.0 - BETA_TWO ** STEP
GRAD_NAMES = ("grad_wq", "grad_wk", "grad_wv", "grad_wo", "grad_gate", "grad_up", "grad_down", "grad_attn_norm", "grad_mlp_norm", "grad_final_norm")


def param_shapes():
    return [(LAYERS, D, Q_DIM), (LAYERS, D, KV_DIM), (LAYERS, D, KV_DIM), (LAYERS, Q_DIM, D), (LAYERS, D, FF), (LAYERS, D, FF), (LAYERS, FF, D), (LAYERS, D), (LAYERS, D), (D,)]


def split_flat(flat_vec):
    tensors = []
    offset = 0
    for piece_shape in param_shapes():
        piece_size = math.prod(piece_shape)
        tensors.append(flat_vec[offset:offset + piece_size].reshape(piece_shape))
        offset += piece_size
    return tensors


def setup_inputs(seed: int = 0) -> dict:
    key_list = jax.random.split(jax.random.key(seed), 15)
    norm_target = 3.0 * jnp.power(3.0, jax.random.uniform(key_list[14], (), jnp.float32))
    grad_scale = norm_target * math.sqrt(DP / TOTAL)
    inputs = {}
    for position, (arg_name, arg_shape) in enumerate(zip(GRAD_NAMES, param_shapes())):
        sample = jax.random.normal(key_list[position], (DP,) + arg_shape, jnp.float32)
        inputs[arg_name] = (grad_scale * sample).astype(jnp.bfloat16)
    valid_mask = (jnp.arange(PADDED) < TOTAL).astype(jnp.float32)
    grad_unit = 1.0 / math.sqrt(TOTAL)
    inputs["master"] = 0.02 * jax.random.normal(key_list[10], (PADDED,), jnp.float32) * valid_mask
    inputs["exp_avg"] = 0.1 * grad_unit * jax.random.normal(key_list[11], (PADDED,), jnp.float32) * valid_mask
    inputs["exp_avg_sq"] = 0.05 * grad_unit * grad_unit * (0.5 + jax.random.uniform(key_list[12], (PADDED,), jnp.float32)) * valid_mask
    inputs["learn_rate"] = 1e-2 * jnp.power(4.0, jax.random.uniform(key_list[13], (), jnp.float32))
    return inputs


def reference(grad_wq, grad_wk, grad_wv, grad_wo, grad_gate, grad_up, grad_down, grad_attn_norm, grad_mlp_norm, grad_final_norm, master, exp_avg, exp_avg_sq, learn_rate):
    local_grads = [grad_wq, grad_wk, grad_wv, grad_wo, grad_gate, grad_up, grad_down, grad_attn_norm, grad_mlp_norm, grad_final_norm]
    pieces = [jnp.sum(local_grad, axis=0, dtype=jnp.float32).reshape(-1) for local_grad in local_grads]
    pieces.append(jnp.zeros((PADDED - TOTAL,), jnp.float32))
    mean_grad = jnp.concatenate(pieces) / DP
    grad_norm = jnp.sqrt(jnp.sum(mean_grad * mean_grad))
    clip_coef = jnp.minimum(1.0, MAX_NORM / (grad_norm + CLIP_EPS))
    clipped = clip_coef * mean_grad
    new_avg = BETA_ONE * exp_avg + (1.0 - BETA_ONE) * clipped
    new_avg_sq = BETA_TWO * exp_avg_sq + (1.0 - BETA_TWO) * clipped * clipped
    decay_mask = (jnp.arange(PADDED) < MATRIX_COUNT).astype(jnp.float32)
    adam_dir = (new_avg / BIAS_ONE) / (jnp.sqrt(new_avg_sq / BIAS_TWO) + ADAM_EPS)
    new_master = master - learn_rate * (WEIGHT_DECAY * decay_mask * master + adam_dir)
    param_wq, param_wk, param_wv, param_wo, param_gate, param_up, param_down, param_attn_norm, param_mlp_norm, param_final_norm = split_flat(new_master[:TOTAL].astype(jnp.bfloat16))
    return (new_master, new_avg, new_avg_sq, param_wq, param_wk, param_wv, param_wo, param_gate, param_up, param_down, param_attn_norm, param_mlp_norm, param_final_norm, grad_norm)
```

```python
import functools
import jax
import jax.numpy as jnp
from jax import lax
from jax.experimental import pallas as pl
from jax.experimental.pallas import tpu as pltpu
from jax.sharding import PartitionSpec as P

BETA_ONE = 0.9
BETA_TWO = 0.95
ADAM_EPS = 1e-8
WEIGHT_DECAY = 0.1
MAX_NORM = 1.0
CLIP_EPS = 1e-6
STEP = 4
BIAS_ONE = 1.0 - BETA_ONE ** STEP
BIAS_TWO = 1.0 - BETA_TWO ** STEP

MESH = pl.DeviceIdType.MESH
LANES = 128
SEG_TILES = 3456
SEG_ROWS = SEG_TILES * 8
LOCAL_ROWS = SEG_ROWS + 6
MATRIX_ROWS = 8 * SEG_ROWS
TAIL = 48
N = 216
ROWS = N * 8
HALF = 8
RING = 4
LAG = 5
WIDTHS = (24, 9, 3)


def neighbours(me):
    core = lax.rem(me, 2)
    x = lax.rem(lax.div(me, 2), 2)
    y = lax.div(me, 4)
    flip = 1 - 2 * core
    xn = me + 2 - 4 * x
    yn = me + 4 - 8 * y
    diag = xn + 4 - 8 * y
    return flip, me + flip, xn, yn, diag


def on_piece(refs, seg, tile, act):
    wq, wk, wv, wo, gate, up, down = refs
    pl.when((seg == 0) & (tile < 2592))(lambda: act(wq, tile))
    pl.when((seg == 0) & (tile >= 2592))(lambda: act(wk, tile - 2592))
    pl.when((seg == 1) & (tile < 864))(lambda: act(wv, tile))
    pl.when((seg == 1) & (tile >= 864))(lambda: act(wo, tile - 864))
    pl.when((seg == 2) | (seg == 3))(lambda: act(gate, (seg - 2) * SEG_TILES + tile))
    pl.when((seg == 4) | (seg == 5))(lambda: act(up, (seg - 4) * SEG_TILES + tile))
    pl.when((seg == 6) | (seg == 7))(lambda: act(down, (seg - 6) * SEG_TILES + tile))


def on_width(seg, tile, act):
    narrow = ((seg == 0) & (tile >= 2592)) | ((seg == 1) & (tile < 864))
    wide = (seg >= 2) & (seg < 6)
    pl.when(wide)(lambda: act(24))
    pl.when(narrow)(lambda: act(3))
    pl.when(jnp.logical_not(wide | narrow))(lambda: act(9))


def load_piece(refs, seg, tile, buf, sem):
    def act(ref, off):
        pltpu.make_async_copy(ref.at[pl.ds(off, N)], buf, sem).start()
    on_piece(refs, seg, tile, act)


def store_piece(refs, seg, tile, buf, sem):
    def act(ref, off):
        pltpu.make_async_copy(buf, ref.at[pl.ds(off, N)], sem).start()
    on_piece(refs, seg, tile, act)


def tiles_loop(body, group=12):
    def step(i, carry):
        body(pl.ds(pl.multiple_of(i * group, group), group))
        return carry
    lax.fori_loop(0, N // group, step, 0)


def remote(src, dst, send, recv, dev):
    return pltpu.make_async_remote_copy(src_ref=src, dst_ref=dst, send_sem=send, recv_sem=recv, device_id=(dev,), device_id_type=MESH)


def greet(devs):
    barrier = pltpu.get_barrier_semaphore()
    for dev in devs:
        pl.semaphore_signal(barrier, inc=1, device_id=(dev,), device_id_type=MESH)
    pl.semaphore_wait(barrier, len(devs))


def reduce_kernel(wq, wk, wv, wo, gate, up, down, gtail, g_out, n_out, land_x, land_y, land_p,
                  raw_p, raw_q, raw_o, got, fwd, stage_p, stage, own_in, own_g, norm_send, norm_land,
                  s_x, s_y, s_p, r_x, r_y, r_p, l_p, l_q, l_o, l_got, l_fwd, l_own, l_g, l_t, s_n, r_n):
    refs = (wq, wk, wv, wo, gate, up, down)
    me = lax.axis_index("dp")
    flip, partner, xn, yn, diag = neighbours(me)
    greet((partner, xn, yn))
    tail_copy = pltpu.make_async_copy(gtail, g_out.at[pl.ds(SEG_ROWS, TAIL)], l_t)
    tail_copy.start()
    n_out[...] = jnp.zeros_like(n_out)

    def job(s, link):
        j = lax.rem(s, HALF)
        first = jnp.where(s < 16, link, 1 - link)
        seg = jnp.where(s < 8, diag, xn if link == 0 else yn)
        return seg, first * (HALF * N) + j * N

    def give(jobs, par, wait_old):
        for a, (seg, tile, slot) in enumerate(jobs):
            load_piece(refs, seg + flip, tile, raw_p.at[a], l_p.at[a])
        for a, (seg, tile, slot) in enumerate(jobs):
            pltpu.make_async_copy(wq.at[pl.ds(0, N)], raw_p.at[a], l_p.at[a]).wait()
            copy = remote(stage_p.at[par, a], land_p.at[slot], s_p.at[par, a], r_p.at[slot], partner)
            pl.when(wait_old)(copy.wait_send)

            def conv(d, a=a):
                stage_p[par, a, d] = raw_p[a, d].astype(jnp.float32)
            tiles_loop(conv)
            copy.start()

    def link_jobs(s):
        return [job(s, link) + (link * 24 + s,) for link in (0, 1)]

    def own_jobs(j):
        return [(me, h * HALF * N + j * N, 48 + h * HALF + j) for h in (0, 1)]

    def fetch(src, buf, sem):
        pltpu.make_async_copy(src, buf, sem).start()

    def fetched(src, buf, sem):
        pltpu.make_async_copy(src, buf, sem).wait()

    give(link_jobs(0), 0, False)

    def step(s, count):
        j = lax.rem(s, HALF)
        more = s < 23
        own_give = (s >= 23) & (s < 31)

        @pl.when(more)
        def _():
            par = lax.rem(s + 1, 2)
            give(link_jobs(s + 1), par, s >= 1)

        @pl.when(s < 24)
        def _():
            ring = lax.rem(s, RING)
            jobs = link_jobs(s)
            for a, (seg, tile, slot) in enumerate(jobs):
                load_piece(refs, seg, tile, raw_q.at[a], l_q.at[a])
            for a, (seg, tile, slot) in enumerate(jobs):
                remote(stage_p.at[0, a], land_p.at[slot], s_p.at[0, a], r_p.at[slot], partner).wait_recv()
                fetch(land_p.at[slot], got.at[a], l_got.at[a])

            @pl.when(s >= 16)
            def _():
                remote(stage.at[0, 0], land_x.at[j], s_x.at[0], r_x.at[j], xn).wait_recv()
                remote(stage.at[0, 1], land_y.at[j], s_y.at[0], r_y.at[j], yn).wait_recv()
                fetch(land_y.at[j], fwd.at[0], l_fwd.at[0])
                fetch(land_x.at[j], fwd.at[1], l_fwd.at[1])
            copies = [remote(stage.at[ring, 0], land_x.at[s], s_x.at[ring], r_x.at[s], xn),
                      remote(stage.at[ring, 1], land_y.at[s], s_y.at[ring], r_y.at[s], yn)]
            for a in (0, 1):
                fetched(wq.at[pl.ds(0, N)], raw_q.at[a], l_q.at[a])
                fetched(land_p.at[0], got.at[a], l_got.at[a])
                pl.when(s >= RING)(copies[a].wait_send)

                @pl.when(s < 16)
                def _(a=a):
                    def add(d):
                        stage[ring, a, d] = raw_q[a, d].astype(jnp.float32) + got[a, d]
                    tiles_loop(add)

                @pl.when(s >= 16)
                def _(a=a):
                    fetched(land_x.at[0], fwd.at[a], l_fwd.at[a])

                    def add(d):
                        stage[ring, a, d] = raw_q[a, d].astype(jnp.float32) + got[a, d] + fwd[a, d]
                    tiles_loop(add)
                copies[a].start()

        @pl.when((s >= 12) & (s < 20))
        def _():
            give_own(s - 12)

        @pl.when(s >= 16 + LAG)
        def _():
            take_own(s - 16 - LAG)
        return count

    def give_own(j):
        for h, (seg, tile, slot) in enumerate(own_jobs(j)):
            load_piece(refs, seg + flip, tile, raw_o.at[h], l_o.at[h])
        for h, (seg, tile, slot) in enumerate(own_jobs(j)):
            fetched(wq.at[pl.ds(0, N)], raw_o.at[h], l_o.at[h])
            copy = remote(stage_p.at[2, h], land_p.at[slot], s_p.at[2, h], r_p.at[slot], partner)
            pl.when(j >= 1)(copy.wait_send)

            def conv(d, h=h):
                stage_p[2, h, d] = raw_o[h, d].astype(jnp.float32)
            tiles_loop(conv)
            copy.start()

    def take_own(j):
        for h, (seg, tile, slot) in enumerate(own_jobs(j)):
            load_piece(refs, seg, tile, raw_o.at[h], l_o.at[h])
            remote(stage_p.at[2, h], land_p.at[slot], s_p.at[2, h], r_p.at[slot], partner).wait_recv()
            fetch(land_p.at[slot], own_in.at[h, 0], l_own.at[h, 0])
        for h in (0, 1):
            one, two = 8 + j, 16 + j
            if h == 0:
                remote(stage.at[0, 0], land_x.at[one], s_x.at[0], r_x.at[one], xn).wait_recv()
                fetch(land_x.at[one], own_in.at[h, 1], l_own.at[h, 1])
            else:
                remote(stage.at[0, 1], land_y.at[one], s_y.at[0], r_y.at[one], yn).wait_recv()
                fetch(land_y.at[one], own_in.at[h, 1], l_own.at[h, 1])
        for h in (0, 1):
            if h == 0:
                remote(stage.at[0, 1], land_y.at[two], s_y.at[0], r_y.at[two], yn).wait_recv()
                fetch(land_y.at[two], own_in.at[h, 2], l_own.at[h, 2])
            else:
                remote(stage.at[0, 0], land_x.at[two], s_x.at[0], r_x.at[two], xn).wait_recv()
                fetch(land_x.at[two], own_in.at[h, 2], l_own.at[h, 2])
        for h, (seg, tile, slot) in enumerate(own_jobs(j)):
            fetched(wq.at[pl.ds(0, N)], raw_o.at[h], l_o.at[h])
            for a in range(3):
                fetched(land_p.at[0], own_in.at[h, a], l_own.at[h, a])
            row = pl.multiple_of(tile * 8, 8)
            out = pltpu.make_async_copy(own_g.at[h], g_out.at[pl.ds(row, ROWS)], l_g.at[h])
            pl.when(j >= 1)(out.wait)

            def relay(width, h=h):
                def body(r, acc):
                    for w in range(width):
                        t = r * width + w
                        g = (raw_o[h, t].astype(jnp.float32) + own_in[h, 0, t] + own_in[h, 1, t] + own_in[h, 2, t]) * 0.125
                        own_g[h, pl.ds(r * (8 * width) + w, 8, stride=width), :] = g
                        acc = acc + g * g
                    return acc
                n_out[...] += lax.fori_loop(0, N // width, body, jnp.zeros((8, LANES), jnp.float32))
            on_width(me, tile, relay)
            out.start()

    lax.fori_loop(0, 24 + LAG, step, 0)

    for r, dev in enumerate((partner, xn, yn)):
        norm_send[r] = n_out[...]
        copy = remote(norm_send.at[r], norm_land.at[r], s_n.at[r], r_n.at[r], dev)
        copy.start()
        copy.wait()
        n_out[...] += norm_land[r]
    tail_copy.wait()
    for a in (0, 1):
        for par in range(3):
            remote(stage_p.at[par, a], land_p.at[0], s_p.at[par, a], r_p.at[0], partner).wait_send()
        pltpu.make_async_copy(own_g.at[a], g_out.at[pl.ds(0, ROWS)], l_g.at[a]).wait()
    for ring in range(RING):
        remote(stage.at[ring, 0], land_x.at[0], s_x.at[ring], r_x.at[0], xn).wait_send()
        remote(stage.at[ring, 1], land_y.at[0], s_y.at[ring], r_y.at[0], yn).wait_send()


def gather_kernel(g_in, p_in, m_in, v_in, head, scal, p_out, m_out, v_out, wq, wk, wv, wo, gate, up, down, land,
                  gb, st, pb, stage, cin, cout, s_x, s_y, s_p, r_x, r_y, r_o, r_px, r_py, f_x, f_y, d_x, d_y,
                  l_in, l_out, l_c, l_o):
    refs = (wq, wk, wv, wo, gate, up, down)
    me = lax.axis_index("dp")
    flip, partner, xn, yn, diag = neighbours(me)
    greet((partner, xn, yn))
    coef, lr = scal[0], scal[1]
    shift = 6 * me
    pb[pl.ds(0, TAIL), :] = head[...]
    ins, outs = (p_in, m_in, v_in), (p_out, m_out, v_out)

    def at(seg, c):
        return land.at[seg, pl.ds(pl.multiple_of(c * N, N), N)]

    def link_piece(q, link):
        seg = jnp.where(q < 16, xn if link == 0 else yn, diag)
        chunk = jnp.where(q < 16, q, q - 8 if link == 0 else q - 16)
        return seg, chunk

    def own(s):
        ring = lax.rem(s, RING)
        row = pl.multiple_of(s * ROWS, 8)
        pltpu.make_async_copy(g_in.at[pl.ds(row, ROWS + TAIL)], gb, l_in.at[3]).start()
        for a in range(3):
            @pl.when(s >= 1)
            def _(a=a):
                pltpu.make_async_copy(st.at[a], outs[a].at[pl.ds(row, ROWS)], l_out.at[a]).wait()
            pltpu.make_async_copy(ins[a].at[pl.ds(row, ROWS)], st.at[a], l_in.at[a]).start()
        pltpu.make_async_copy(g_in.at[pl.ds(row, ROWS + TAIL)], gb, l_in.at[3]).wait()
        for a in range(3):
            pltpu.make_async_copy(ins[a].at[pl.ds(row, ROWS)], st.at[a], l_in.at[a]).wait()
        slab = 48
        base = me * LOCAL_ROWS + s * ROWS

        def update(i, carry):
            d = pl.ds(pl.multiple_of(i * slab, 8), slab)
            e = pl.ds(i * slab + shift, slab)
            g = gb[e, :] * coef
            p = st[0, d, :]
            m = BETA_ONE * st[1, d, :] + (1.0 - BETA_ONE) * g
            v = BETA_TWO * st[2, d, :] + (1.0 - BETA_TWO) * g * g
            direction = (m * (1.0 / BIAS_ONE)) / (jnp.sqrt(v * (1.0 / BIAS_TWO)) + ADAM_EPS)
            place = lax.broadcasted_iota(jnp.int32, (slab, LANES), 0) + (base + i * slab)
            decay = jnp.where(place < MATRIX_ROWS, WEIGHT_DECAY * p, 0.0)
            p = p - lr * (decay + direction)
            st[0, d, :] = p
            st[1, d, :] = m
            st[2, d, :] = v
            pb[e, :] = p
            return carry
        lax.fori_loop(0, ROWS // slab, update, 0)
        for a in range(3):
            pltpu.make_async_copy(st.at[a], outs[a].at[pl.ds(row, ROWS)], l_out.at[a]).start()
        copies = [remote(stage.at[ring], at(me, s), s_x.at[ring], r_x.at[s], xn),
                  remote(stage.at[ring], at(me, s), s_y.at[ring], r_y.at[s], yn),
                  remote(stage.at[ring], at(me, s), s_p.at[ring], r_o.at[s], partner)]

        @pl.when(s >= RING)
        def _():
            for copy in copies:
                copy.wait_send()

        def relay(width):
            def body(r, carry):
                for w in range(width):
                    t = r * width + w
                    stage[ring, t] = pb[pl.ds(r * (8 * width) + w, 8, stride=width), :]
                return carry
            lax.fori_loop(0, N // width, body, 0)
        on_width(me, s * N, relay)
        pb[pl.ds(0, TAIL), :] = pb[pl.ds(ROWS, TAIL), :]
        for copy in copies:
            copy.start()

        def conv(d):
            cout[0, d] = stage[ring, d].astype(jnp.bfloat16)
        tiles_loop(conv)
        store_piece(refs, me, s * N, cout.at[0], l_o.at[0])

    def convert(slot, seg, chunk):
        pltpu.make_async_copy(at(0, 0), cin.at[slot - 1], l_c.at[slot - 1]).wait()

        def conv(d):
            cout[slot, d] = cin[slot - 1, d].astype(jnp.bfloat16)
        tiles_loop(conv)
        store_piece(refs, seg, chunk * N, cout.at[slot], l_o.at[slot])

    def fetch(slot, seg, chunk):
        pltpu.make_async_copy(at(seg, chunk), cin.at[slot - 1], l_c.at[slot - 1]).start()

    def stored(slot):
        pltpu.make_async_copy(cout.at[slot], wq.at[pl.ds(0, N)], l_o.at[slot]).wait()

    def step(s, carry):
        j = s - 16
        q = s - LAG
        q2 = s - LAG - 1

        @pl.when((s >= 1) & (s <= 16))
        def _():
            stored(0)

        @pl.when(s < 16)
        def _():
            own(s)

        @pl.when((s >= 16) & (s < 24))
        def _():
            remote(at(xn, j), at(xn, j), f_y.at[j], r_y.at[s], yn).start()
            remote(at(yn, 8 + j), at(yn, 8 + j), f_x.at[j], r_x.at[s], xn).start()

        @pl.when((q >= 1) & (q <= 24))
        def _():
            stored(1)
            stored(2)

        @pl.when((q2 >= 1) & (q2 <= 24))
        def _():
            stored(3)
            stored(4)

        @pl.when((q2 >= 1) & (q2 <= 16))
        def _():
            stored(5)

        xseg, xc = link_piece(q, 0)
        yseg, yc = link_piece(q, 1)
        par = lax.rem(s, 2)

        @pl.when((q >= 0) & (q < 24))
        def _():
            remote(at(xseg, xc), at(xseg, xc), d_x.at[par], r_x.at[q], xn).wait_recv()
            copy = remote(at(xseg, xc), at(xseg, xc), d_x.at[par], r_px.at[q], partner)
            pl.when(q >= 2)(copy.wait_send)
            copy.start()
            fetch(1, xseg, xc)
            remote(at(yseg, yc), at(yseg, yc), d_y.at[par], r_y.at[q], yn).wait_recv()
            copy = remote(at(yseg, yc), at(yseg, yc), d_y.at[par], r_py.at[q], partner)
            pl.when(q >= 2)(copy.wait_send)
            copy.start()
            fetch(2, yseg, yc)

        pxseg, pxc = link_piece(q2, 0)
        pyseg, pyc = link_piece(q2, 1)

        @pl.when((q2 >= 0) & (q2 < 16))
        def _():
            remote(at(partner, q2), at(partner, q2), s_p.at[0], r_o.at[q2], partner).wait_recv()
            fetch(5, partner, q2)

        @pl.when((q2 >= 0) & (q2 < 24))
        def _():
            remote(at(0, 0), at(0, 0), d_x.at[par], r_px.at[q2], partner).wait_recv()
            fetch(3, pxseg + flip, pxc)
            remote(at(0, 0), at(0, 0), d_y.at[par], r_py.at[q2], partner).wait_recv()
            fetch(4, pyseg + flip, pyc)

        @pl.when((q >= 0) & (q < 24))
        def _():
            convert(1, xseg, xc)
            convert(2, yseg, yc)

        @pl.when((q2 >= 0) & (q2 < 16))
        def _():
            convert(5, partner, q2)

        @pl.when((q2 >= 0) & (q2 < 24))
        def _():
            convert(3, pxseg + flip, pxc)
            convert(4, pyseg + flip, pyc)
        return carry

    lax.fori_loop(0, 24 + LAG + 1, step, 0)
    stored(3)
    stored(4)
    for a in range(3):
        pltpu.make_async_copy(st.at[a], outs[a].at[pl.ds(0, ROWS)], l_out.at[a]).wait()
    for ring in range(RING):
        remote(stage.at[ring], at(me, 0), s_x.at[ring], r_x.at[0], xn).wait_send()
        remote(stage.at[ring], at(me, 0), s_y.at[ring], r_y.at[0], yn).wait_send()
        remote(stage.at[ring], at(me, 0), s_p.at[ring], r_o.at[0], partner).wait_send()
    for j in range(HALF):
        remote(at(0, 0), at(0, 0), f_y.at[j], r_y.at[0], yn).wait_send()
        remote(at(0, 0), at(0, 0), f_x.at[j], r_x.at[0], xn).wait_send()
    for par in (0, 1):
        remote(at(0, 0), at(0, 0), d_x.at[par], r_px.at[0], partner).wait_send()
        remote(at(0, 0), at(0, 0), d_y.at[par], r_py.at[0], partner).wait_send()


ANY = pl.BlockSpec(memory_space=pl.ANY)
VMEM = pl.BlockSpec(memory_space=pltpu.VMEM)
SMEM = pl.BlockSpec(memory_space=pltpu.SMEM)
F32 = jnp.float32
BF16 = jnp.bfloat16
LIMIT = 62 * 1024 * 1024


def to_tiles(x):
    rows, cols = x.shape[-2:]
    lead = x.size // cols
    return x.reshape(lead // 8, 8, cols // LANES, LANES).transpose(0, 2, 1, 3).reshape(-1, 8, LANES)


def from_tiles(t, shape):
    cols = shape[-1]
    lead = t.size // cols
    return t.reshape(lead // 8, cols // LANES, 8, LANES).transpose(0, 2, 1, 3).reshape(shape)


def reduce_call(tiles, gtail):
    dma = pltpu.SemaphoreType.DMA
    chunk = (N, 8, LANES)
    return pl.pallas_call(
        reduce_kernel,
        out_shape=[jax.ShapeDtypeStruct((SEG_ROWS + TAIL, LANES), F32), jax.ShapeDtypeStruct((8, LANES), F32),
                   jax.ShapeDtypeStruct((24,) + chunk, F32), jax.ShapeDtypeStruct((24,) + chunk, F32),
                   jax.ShapeDtypeStruct((64,) + chunk, F32)],
        in_specs=[ANY] * 7 + [VMEM],
        out_specs=[ANY, VMEM, ANY, ANY, ANY],
        scratch_shapes=[pltpu.VMEM((2,) + chunk, BF16), pltpu.VMEM((2,) + chunk, BF16), pltpu.VMEM((2,) + chunk, BF16),
                        pltpu.VMEM((2,) + chunk, F32), pltpu.VMEM((2,) + chunk, F32), pltpu.VMEM((3, 2) + chunk, F32),
                        pltpu.VMEM((RING, 2) + chunk, F32), pltpu.VMEM((2, 3) + chunk, F32), pltpu.VMEM((2, ROWS, LANES), F32),
                        pltpu.VMEM((3, 8, LANES), F32), pltpu.VMEM((3, 8, LANES), F32),
                        dma((RING,)), dma((RING,)), dma((3, 2)), dma((24,)), dma((24,)), dma((64,)),
                        dma((2,)), dma((2,)), dma((2,)), dma((2,)), dma((2,)), dma((2, 3)), dma((2,)), dma, dma((3,)), dma((3,))],
        compiler_params=pltpu.CompilerParams(collective_id=0, has_side_effects=True, vmem_limit_bytes=LIMIT),
        name="reduce_grads",
    )(*tiles, gtail)


def gather_call(g, p, m, v, head, scal):
    dma = pltpu.SemaphoreType.DMA
    chunk = (N, 8, LANES)
    flat = jax.ShapeDtypeStruct((LOCAL_ROWS, LANES), F32)
    tile_counts = (2592, 864, 864, 2592, 6912, 6912, 6912)
    return pl.pallas_call(
        gather_kernel,
        out_shape=[flat] * 3 + [jax.ShapeDtypeStruct((c, 8, LANES), BF16) for c in tile_counts]
        + [jax.ShapeDtypeStruct((8, SEG_TILES, 8, LANES), F32)],
        in_specs=[ANY] * 4 + [VMEM, SMEM],
        out_specs=[ANY] * 11,
        scratch_shapes=[pltpu.VMEM((ROWS + TAIL, LANES), F32), pltpu.VMEM((3, ROWS, LANES), F32), pltpu.VMEM((ROWS + TAIL, LANES), F32),
                        pltpu.VMEM((RING,) + chunk, F32), pltpu.VMEM((5,) + chunk, F32), pltpu.VMEM((6,) + chunk, BF16),
                        dma((RING,)), dma((RING,)), dma((RING,)), dma((24,)), dma((24,)), dma((16,)), dma((24,)), dma((24,)),
                        dma((HALF,)), dma((HALF,)), dma((2,)), dma((2,)), dma((4,)), dma((3,)), dma((5,)), dma((6,))],
        compiler_params=pltpu.CompilerParams(collective_id=1, has_side_effects=True, vmem_limit_bytes=LIMIT),
        name="update_gather",
    )(g, p, m, v, head, scal)


def adam(g, p, m, v, lr, decay):
    m = BETA_ONE * m + (1.0 - BETA_ONE) * g
    v = BETA_TWO * v + (1.0 - BETA_TWO) * g * g
    direction = (m / BIAS_ONE) / (jnp.sqrt(v / BIAS_TWO) + ADAM_EPS)
    return p - lr * (decay * p + direction), m, v


def local_step(*arrays):
    grads = arrays[:10]
    master, exp_avg, exp_avg_sq, lr = arrays[10:]
    me = lax.axis_index("dp")
    wq, wk, wv, wo, gate, up, down = grads[:7]
    width = TAIL * LANES
    gains = jnp.concatenate([g.reshape(-1) for g in grads[7:]] + [jnp.zeros((width - 5760,), BF16)])
    firsts = [wv[0, 0, :16], gate[0, 0, :2], gate[0, 1, :2], up[0, 0, :2], up[0, 1, :2], down[0, 0, :6], down[0, 1, :6]]
    heads = jnp.stack([f.reshape(-1)[:width] for f in firsts] + [gains]).astype(F32) * 0.125
    gt = lax.psum(heads, "dp").reshape(8, TAIL, LANES)
    window = jnp.stack([a[-width:] for a in (master, exp_avg, exp_avg_sq)])
    window = jnp.pad(window, ((0, 0), (0, width)))
    window = lax.dynamic_slice(window, (0, (42 - 6 * me) * LANES), (3, width))
    tails = lax.all_gather(window, "dp").reshape(8, 3, TAIL, LANES)
    gtail = lax.dynamic_index_in_dim(gt, me, 0, keepdims=False)

    g, squares = reduce_call([to_tiles(x) for x in grads[:7]], gtail)[:2]
    norm = jnp.sqrt(jnp.sum(squares) + jnp.sum(gt[7] * gt[7]))
    coef = jnp.minimum(1.0, MAX_NORM / (norm + CLIP_EPS))
    decay = jnp.where(lax.broadcasted_iota(jnp.int32, (8, TAIL, LANES), 0) < 7, WEIGHT_DECAY, 0.0)
    new_tails = adam(coef * gt, tails[:, 0], tails[:, 1], tails[:, 2], lr, decay)
    head = lax.dynamic_index_in_dim(new_tails[0], lax.rem(me + 7, 8), 0, keepdims=False)
    res = gather_call(g, *[a.reshape(LOCAL_ROWS, LANES) for a in (master, exp_avg, exp_avg_sq)], head, jnp.stack([coef, lr]))
    states = []
    for full, tail in zip(res[:3], new_tails):
        last = lax.dynamic_slice(tail, (me, 6 * me, 0), (1, 6, LANES))[0]
        states.append(lax.dynamic_update_slice(full, last, (SEG_ROWS, 0)).reshape(-1))
    params = [from_tiles(t, x.shape[1:]) for t, x in zip(res[3:10], grads[:7])]
    gains = new_tails[0][7].reshape(-1).astype(BF16)
    params += [gains[:2304].reshape(2, 1152), gains[2304:4608].reshape(2, 1152), gains[4608:5760]]
    return tuple(states + params + [norm])


def solution(mesh):
    return jax.shard_map(local_step, mesh=mesh, in_specs=(P("dp"),) * 13 + (P(),), out_specs=(P("dp"),) * 3 + (P(),) * 11, check_vma=False)
```

```python
import functools
import jax
import jax.numpy as jnp
from jax import lax
from jax.experimental import pallas as pl
from jax.experimental.pallas import tpu as pltpu
from jax.sharding import PartitionSpec as P

BETA_ONE = 0.9
BETA_TWO = 0.95
ADAM_EPS = 1e-8
WEIGHT_DECAY = 0.1
MAX_NORM = 1.0
CLIP_EPS = 1e-6
STEP = 4
BIAS_ONE = 1.0 - BETA_ONE ** STEP
BIAS_TWO = 1.0 - BETA_TWO ** STEP

MESH = pl.DeviceIdType.MESH
LANES = 128
SEG_TILES = 3456
SEG_ROWS = SEG_TILES * 8
LOCAL_ROWS = SEG_ROWS + 6
MATRIX_ROWS = 8 * SEG_ROWS
TAIL = 48
N = 216
ROWS = N * 8
HALF = 8
RING = 4
LAG = 5
WIDTHS = (24, 9, 3)


def neighbours(me):
    core = lax.rem(me, 2)
    x = lax.rem(lax.div(me, 2), 2)
    y = lax.div(me, 4)
    flip = 1 - 2 * core
    xn = me + 2 - 4 * x
    yn = me + 4 - 8 * y
    diag = xn + 4 - 8 * y
    return flip, me + flip, xn, yn, diag


def on_piece(refs, seg, tile, act):
    wq, wk, wv, wo, gate, up, down = refs
    pl.when((seg == 0) & (tile < 2592))(lambda: act(wq, tile))
    pl.when((seg == 0) & (tile >= 2592))(lambda: act(wk, tile - 2592))
    pl.when((seg == 1) & (tile < 864))(lambda: act(wv, tile))
    pl.when((seg == 1) & (tile >= 864))(lambda: act(wo, tile - 864))
    pl.when((seg == 2) | (seg == 3))(lambda: act(gate, (seg - 2) * SEG_TILES + tile))
    pl.when((seg == 4) | (seg == 5))(lambda: act(up, (seg - 4) * SEG_TILES + tile))
    pl.when((seg == 6) | (seg == 7))(lambda: act(down, (seg - 6) * SEG_TILES + tile))


def on_width(seg, tile, act):
    narrow = ((seg == 0) & (tile >= 2592)) | ((seg == 1) & (tile < 864))
    wide = (seg >= 2) & (seg < 6)
    pl.when(wide)(lambda: act(24))
    pl.when(narrow)(lambda: act(3))
    pl.when(jnp.logical_not(wide | narrow))(lambda: act(9))


def load_piece(refs, seg, tile, buf, sem):
    def act(ref, off):
        pltpu.make_async_copy(ref.at[pl.ds(off, N)], buf, sem).start()
    on_piece(refs, seg, tile, act)


def store_piece(refs, seg, tile, buf, sem):
    def act(ref, off):
        pltpu.make_async_copy(buf, ref.at[pl.ds(off, N)], sem).start()
    on_piece(refs, seg, tile, act)


def tiles_loop(body, group=12):
    def step(i, carry):
        body(pl.ds(pl.multiple_of(i * group, group), group))
        return carry
    lax.fori_loop(0, N // group, step, 0)


def remote(src, dst, send, recv, dev):
    return pltpu.make_async_remote_copy(src_ref=src, dst_ref=dst, send_sem=send, recv_sem=recv, device_id=(dev,), device_id_type=MESH)


def greet(devs):
    barrier = pltpu.get_barrier_semaphore()
    for dev in devs:
        pl.semaphore_signal(barrier, inc=1, device_id=(dev,), device_id_type=MESH)
    pl.semaphore_wait(barrier, len(devs))


FRONT = ((2, 0, 6, 3), (4, 0, 24, 24), (4, SEG_TILES, 24, 24), (5, 0, 24, 24), (5, SEG_TILES, 24, 24), (6, 0, 9, 9), (6, SEG_TILES, 9, 9))
WIN = 27600
WIN_ROWS = LOCAL_ROWS - WIN


def adam(g, p, m, v, lr, decay):
    m = BETA_ONE * m + (1.0 - BETA_ONE) * g
    v = BETA_TWO * v + (1.0 - BETA_TWO) * g * g
    direction = (m * (1.0 / BIAS_ONE)) / (jnp.sqrt(v * (1.0 / BIAS_TWO)) + ADAM_EPS)
    return p - lr * (decay * p + direction), m, v


def step_kernel(wq, wk, wv, wo, gate, up, down, g_attn, g_mlp, g_final, p_in, m_in, v_in, rate,
                p_out, m_out, v_out, o_wq, o_wk, o_wv, o_wo, o_gate, o_up, o_down, o_attn, o_mlp, o_final, o_norm,
                g_flat, land_x, land_y, land_p, land,
                raw_p, raw_q, raw_o, got, fwd, stage_p, stage, own_in, own_g, norm_send, norm_land, n_out,
                front_raw, front, front_land, tail_g, window, halo, window_g, gains_send, gains_land, coef_ref,
                gb, st, pb, stage_u, cin, cout,
                s_x, s_y, s_p, r_x, r_y, r_p, l_p, l_q, l_o, l_got, l_fwd, l_own, l_g, s_n, r_n,
                l_front, s_front, r_front, l_win, s_win, r_win, l_tail, l_six, s_gain, r_gain,
                su_x, su_y, su_p, ru_x, ru_y, ru_o, r_px, r_py, f_x, f_y, d_x, d_y, l_in, l_out, l_c, l_so):
    refs = (wq, wk, wv, wo, gate, up, down)
    outs7 = (o_wq, o_wk, o_wv, o_wo, o_gate, o_up, o_down)
    me = lax.axis_index("dp")
    flip, partner, xn, yn, diag = neighbours(me)
    others = [lax.rem(me + o, 8) for o in range(1, 8)]
    shift = 6 * me
    lr = rate[0]
    ins, outs = (p_in, m_in, v_in), (p_out, m_out, v_out)
    n_out[...] = jnp.zeros_like(n_out)
    window[...] = jnp.zeros_like(window)
    window_g[...] = jnp.zeros_like(window_g)
    halo[:, pl.ds(56, 48), :] = jnp.zeros((3, 48, LANES), jnp.float32)
    front[7] = jnp.zeros(front.shape[1:], jnp.float32)
    greet(others)

    def window_copies():
        out = []
        for a in range(3):
            out.append(pltpu.make_async_copy(ins[a].at[pl.ds(WIN, 48)], window.at[a, pl.ds(0, 48)], l_win.at[a]))
            out.append(pltpu.make_async_copy(ins[a].at[pl.ds(SEG_ROWS, 6)], window.at[a, pl.ds(48, 6)], l_win.at[3 + a]))
        return out

    def front_copies():
        return [pltpu.make_async_copy(refs[k].at[pl.ds(off, cnt)], front_raw.at[d, pl.ds(0, cnt)], l_front.at[d])
                for d, (k, off, cnt, width) in enumerate(FRONT)]

    def front_sends():
        return [remote(front.at[dev, pl.ds(0, TAIL)], front_land.at[o], s_front.at[o], r_front.at[o], dev) for o, dev in enumerate(others)]

    def window_send():
        return remote(window, halo.at[:, pl.ds(0, 56)], s_win, r_win, others[0])

    def small_exchange():
        for copy in window_copies() + front_copies():
            copy.start()
        rows = [(g_attn[0], 2), (g_mlp[0], 2), (g_final[...], 1)]
        place = 0
        for value, count in rows:
            value = value.astype(jnp.float32)
            for r in range(count):
                for w in range(9):
                    front[7, pl.ds(place, 1), :] = value[r:r + 1, w * LANES:(w + 1) * LANES]
                    place += 1
        for copy in window_copies() + front_copies():
            copy.wait()
        for d, (k, off, cnt, width) in enumerate(FRONT):
            for t in range(cnt):
                front[d, pl.ds(t // width * 8 * width + t % width, 8, stride=width), :] = front_raw[d, t].astype(jnp.float32)
        window_send().start()
        for copy in front_sends():
            copy.start()

    def small_finish():
        total = front[me, pl.ds(0, TAIL), :]
        for o, copy in enumerate(front_sends()):
            copy.wait()
            total = total + front_land[o]
        window_send().wait()
        total = total * 0.125
        tail_g[...] = total

        @pl.when(me == 7)
        def _():
            n_out[...] += jnp.sum((total * total).reshape(TAIL // 8, 8, LANES), axis=0)
        copy = pltpu.make_async_copy(tail_g, g_flat.at[pl.ds(SEG_ROWS, TAIL)], l_tail)
        copy.start()
        copy.wait()

    def state_loads(s):
        row = pl.multiple_of(s * ROWS, 8)
        for a in range(3):
            pltpu.make_async_copy(ins[a].at[pl.ds(row, ROWS)], st.at[a], l_in.at[a]).start()

    def gradient_load(s):
        row = pl.multiple_of(s * ROWS, 8)
        pltpu.make_async_copy(g_flat.at[pl.ds(row, ROWS + TAIL)], gb, l_in.at[3]).start()

    def job(s, link):
        j = lax.rem(s, HALF)
        first = jnp.where(s < 16, link, 1 - link)
        seg = jnp.where(s < 8, diag, xn if link == 0 else yn)
        return seg, first * (HALF * N) + j * N

    def give(jobs, par, wait_old):
        for a, (seg, tile, slot) in enumerate(jobs):
            load_piece(refs, seg + flip, tile, raw_p.at[a], l_p.at[a])
        for a, (seg, tile, slot) in enumerate(jobs):
            pltpu.make_async_copy(wq.at[pl.ds(0, N)], raw_p.at[a], l_p.at[a]).wait()
            copy = remote(stage_p.at[par, a], land_p.at[slot], s_p.at[par, a], r_p.at[slot], partner)
            pl.when(wait_old)(copy.wait_send)

            def conv(d, a=a):
                stage_p[par, a, d] = raw_p[a, d].astype(jnp.float32)
            tiles_loop(conv)
            copy.start()

    def link_jobs(s):
        return [job(s, link) + (link * 24 + s,) for link in (0, 1)]

    def own_jobs(j):
        return [(me, h * HALF * N + j * N, 48 + h * HALF + j) for h in (0, 1)]

    def fetch(src, buf, sem):
        pltpu.make_async_copy(src, buf, sem).start()

    def fetched(src, buf, sem):
        pltpu.make_async_copy(src, buf, sem).wait()

    give(link_jobs(0), 0, False)

    def step(s, count):
        j = lax.rem(s, HALF)
        more = s < 23

        @pl.when(more)
        def _():
            par = lax.rem(s + 1, 2)
            give(link_jobs(s + 1), par, s >= 1)

        @pl.when(s < 24)
        def _():
            ring = lax.rem(s, RING)
            jobs = link_jobs(s)
            for a, (seg, tile, slot) in enumerate(jobs):
                load_piece(refs, seg, tile, raw_q.at[a], l_q.at[a])
            for a, (seg, tile, slot) in enumerate(jobs):
                remote(stage_p.at[0, a], land_p.at[slot], s_p.at[0, a], r_p.at[slot], partner).wait_recv()
                fetch(land_p.at[slot], got.at[a], l_got.at[a])

            @pl.when(s >= 16)
            def _():
                remote(stage.at[0, 0], land_x.at[j], s_x.at[0], r_x.at[j], xn).wait_recv()
                remote(stage.at[0, 1], land_y.at[j], s_y.at[0], r_y.at[j], yn).wait_recv()
                fetch(land_y.at[j], fwd.at[0], l_fwd.at[0])
                fetch(land_x.at[j], fwd.at[1], l_fwd.at[1])
            copies = [remote(stage.at[ring, 0], land_x.at[s], s_x.at[ring], r_x.at[s], xn),
                      remote(stage.at[ring, 1], land_y.at[s], s_y.at[ring], r_y.at[s], yn)]
            for a in (0, 1):
                fetched(wq.at[pl.ds(0, N)], raw_q.at[a], l_q.at[a])
                fetched(land_p.at[0], got.at[a], l_got.at[a])
                pl.when(s >= RING)(copies[a].wait_send)

                @pl.when(s < 16)
                def _(a=a):
                    def add(d):
                        stage[ring, a, d] = raw_q[a, d].astype(jnp.float32) + got[a, d]
                    tiles_loop(add)

                @pl.when(s >= 16)
                def _(a=a):
                    fetched(land_x.at[0], fwd.at[a], l_fwd.at[a])

                    def add(d):
                        stage[ring, a, d] = raw_q[a, d].astype(jnp.float32) + got[a, d] + fwd[a, d]
                    tiles_loop(add)
                copies[a].start()

        pl.when(s == 2)(small_exchange)
        pl.when(s == 20)(small_finish)

        @pl.when((s >= 12) & (s < 20))
        def _():
            give_own(s - 12)

        @pl.when(s >= 16 + LAG)
        def _():
            take_own(s - 16 - LAG)
        return count

    def give_own(j):
        for h, (seg, tile, slot) in enumerate(own_jobs(j)):
            load_piece(refs, seg + flip, tile, raw_o.at[h], l_o.at[h])
        for h, (seg, tile, slot) in enumerate(own_jobs(j)):
            fetched(wq.at[pl.ds(0, N)], raw_o.at[h], l_o.at[h])
            copy = remote(stage_p.at[2, h], land_p.at[slot], s_p.at[2, h], r_p.at[slot], partner)
            pl.when(j >= 1)(copy.wait_send)

            def conv(d, h=h):
                stage_p[2, h, d] = raw_o[h, d].astype(jnp.float32)
            tiles_loop(conv)
            copy.start()

    def take_own(j):
        for h, (seg, tile, slot) in enumerate(own_jobs(j)):
            load_piece(refs, seg, tile, raw_o.at[h], l_o.at[h])
            remote(stage_p.at[2, h], land_p.at[slot], s_p.at[2, h], r_p.at[slot], partner).wait_recv()
            fetch(land_p.at[slot], own_in.at[h, 0], l_own.at[h, 0])
        for h in (0, 1):
            one, two = 8 + j, 16 + j
            if h == 0:
                remote(stage.at[0, 0], land_x.at[one], s_x.at[0], r_x.at[one], xn).wait_recv()
                fetch(land_x.at[one], own_in.at[h, 1], l_own.at[h, 1])
            else:
                remote(stage.at[0, 1], land_y.at[one], s_y.at[0], r_y.at[one], yn).wait_recv()
                fetch(land_y.at[one], own_in.at[h, 1], l_own.at[h, 1])
        for h in (0, 1):
            if h == 0:
                remote(stage.at[0, 1], land_y.at[two], s_y.at[0], r_y.at[two], yn).wait_recv()
                fetch(land_y.at[two], own_in.at[h, 2], l_own.at[h, 2])
            else:
                remote(stage.at[0, 0], land_x.at[two], s_x.at[0], r_x.at[two], xn).wait_recv()
                fetch(land_x.at[two], own_in.at[h, 2], l_own.at[h, 2])
        for h, (seg, tile, slot) in enumerate(own_jobs(j)):
            fetched(wq.at[pl.ds(0, N)], raw_o.at[h], l_o.at[h])
            for a in range(3):
                fetched(land_p.at[0], own_in.at[h, a], l_own.at[h, a])
            row = pl.multiple_of(tile * 8, 8)
            out = pltpu.make_async_copy(own_g.at[h], g_flat.at[pl.ds(row, ROWS)], l_g.at[h])
            pl.when(j >= 1)(out.wait)

            def relay(width, h=h):
                def body(r, acc):
                    for w in range(width):
                        t = r * width + w
                        g = (raw_o[h, t].astype(jnp.float32) + own_in[h, 0, t] + own_in[h, 1, t] + own_in[h, 2, t]) * 0.125
                        own_g[h, pl.ds(r * (8 * width) + w, 8, stride=width), :] = g
                        acc = acc + g * g
                    return acc
                n_out[...] += lax.fori_loop(0, N // width, body, jnp.zeros((8, LANES), jnp.float32))
            on_width(me, tile, relay)
            out.start()

    lax.fori_loop(0, 24 + LAG, step, 0)

    state_loads(0)

    for r, dev in enumerate((partner, xn, yn)):
        norm_send[r] = n_out[...]
        copy = remote(norm_send.at[r], norm_land.at[r], s_n.at[r], r_n.at[r], dev)
        copy.start()
        copy.wait()
        n_out[...] += norm_land[r]
    for h in (0, 1):
        pltpu.make_async_copy(own_g.at[h], g_flat.at[pl.ds(0, ROWS)], l_g.at[h]).wait()
    gradient_load(0)
    norm = jnp.sqrt(jnp.sum(n_out[...], axis=(0, 1), keepdims=True))
    o_norm[...] = jnp.broadcast_to(norm, (8, LANES))
    coef_ref[...] = jnp.broadcast_to(jnp.minimum(1.0, MAX_NORM / (norm + CLIP_EPS)), (8, LANES))
    copy = pltpu.make_async_copy(g_flat.at[pl.ds(WIN, 96)], window_g.at[pl.ds(0, 96)], l_tail)
    copy.start()
    copy.wait()
    coef = coef_ref[pl.ds(0, 1), :]

    def state_tail():
        place = lax.broadcasted_iota(jnp.int32, (56, LANES), 0) + (me * LOCAL_ROWS + WIN)
        decay = jnp.where(place < MATRIX_ROWS, WEIGHT_DECAY, 0.0)
        new = adam(window_g[pl.ds(shift, 56), :] * coef, window[0], window[1], window[2], lr, decay)
        for a in range(3):
            window[a] = new[a]
        gains_send[...] = new[0]
        for a in range(3):
            pltpu.make_async_copy(window.at[a, pl.ds(48, 6)], outs[a].at[pl.ds(SEG_ROWS, 6)], l_six.at[a]).start()

        @pl.when(me == 7)
        def _():
            for o, dev in enumerate(others):
                remote(gains_send, gains_land, s_gain.at[o], r_gain, dev).start()

    def gains_finish():
        def write(src):
            t = src[...]

            def row(first):
                return jnp.concatenate([t[first + w:first + w + 1, :] for w in range(9)], axis=1)
            o_attn[...] = jnp.concatenate([row(6), row(15)], axis=0).astype(jnp.bfloat16)
            o_mlp[...] = jnp.concatenate([row(24), row(33)], axis=0).astype(jnp.bfloat16)
            o_final[...] = row(42).astype(jnp.bfloat16)

        @pl.when(me == 7)
        def _():
            for o, dev in enumerate(others):
                remote(gains_send, gains_land, s_gain.at[o], r_gain, dev).wait_send()
            write(gains_send)

        @pl.when(me != 7)
        def _():
            remote(gains_send, gains_land, s_gain.at[0], r_gain, others[0]).wait_recv()
            write(gains_land)
        for a in range(3):
            pltpu.make_async_copy(window.at[a, pl.ds(48, 6)], outs[a].at[pl.ds(SEG_ROWS, 6)], l_six.at[a]).wait()

    def first_rows():
        part = pl.ds(54 - shift, TAIL)
        pb[pl.ds(0, TAIL), :] = adam(gb[pl.ds(0, TAIL), :] * coef, halo[0, part, :], halo[1, part, :], halo[2, part, :], lr, WEIGHT_DECAY)[0]

    for a in (0, 1):
        for par in range(3):
            remote(stage_p.at[par, a], land_p.at[0], s_p.at[par, a], r_p.at[0], partner).wait_send()
    for ring in range(RING):
        remote(stage.at[ring, 0], land_x.at[0], s_x.at[ring], r_x.at[0], xn).wait_send()
        remote(stage.at[ring, 1], land_y.at[0], s_y.at[ring], r_y.at[0], yn).wait_send()

    def at(seg, c):
        return land.at[seg, pl.ds(pl.multiple_of(c * N, N), N)]

    def link_piece(q, link):
        seg = jnp.where(q < 16, xn if link == 0 else yn, diag)
        chunk = jnp.where(q < 16, q, q - 8 if link == 0 else q - 16)
        return seg, chunk

    def own(s):
        ring = lax.rem(s, RING)
        row = pl.multiple_of(s * ROWS, 8)

        @pl.when(s >= 1)
        def _():
            gradient_load(s)
            for a in range(3):
                pltpu.make_async_copy(st.at[a], outs[a].at[pl.ds(row, ROWS)], l_out.at[a]).wait()
            state_loads(s)
        pltpu.make_async_copy(g_flat.at[pl.ds(row, ROWS + TAIL)], gb, l_in.at[3]).wait()
        for a in range(3):
            pltpu.make_async_copy(ins[a].at[pl.ds(row, ROWS)], st.at[a], l_in.at[a]).wait()
        pl.when(s == 0)(first_rows)
        slab = 48
        base = me * LOCAL_ROWS + s * ROWS

        def update(i, carry):
            d = pl.ds(pl.multiple_of(i * slab, 8), slab)
            e = pl.ds(i * slab + shift, slab)
            place = lax.broadcasted_iota(jnp.int32, (slab, LANES), 0) + (base + i * slab)
            decay = jnp.where(place < MATRIX_ROWS, WEIGHT_DECAY, 0.0)
            p, m, v = adam(gb[e, :] * coef, st[0, d, :], st[1, d, :], st[2, d, :], lr, decay)
            st[0, d, :] = p
            st[1, d, :] = m
            st[2, d, :] = v
            pb[e, :] = p
            return carry
        lax.fori_loop(0, ROWS // slab, update, 0)
        for a in range(3):
            pltpu.make_async_copy(st.at[a], outs[a].at[pl.ds(row, ROWS)], l_out.at[a]).start()
        copies = [remote(stage_u.at[ring], at(me, s), su_x.at[ring], ru_x.at[s], xn),
                  remote(stage_u.at[ring], at(me, s), su_y.at[ring], ru_y.at[s], yn),
                  remote(stage_u.at[ring], at(me, s), su_p.at[ring], ru_o.at[s], partner)]

        @pl.when(s >= RING)
        def _():
            for copy in copies:
                copy.wait_send()

        def relay(width):
            def body(r, carry):
                for w in range(width):
                    t = r * width + w
                    stage_u[ring, t] = pb[pl.ds(r * (8 * width) + w, 8, stride=width), :]
                return carry
            lax.fori_loop(0, N // width, body, 0)
        on_width(me, s * N, relay)
        pb[pl.ds(0, TAIL), :] = pb[pl.ds(ROWS, TAIL), :]
        for copy in copies:
            copy.start()

        def conv(d):
            cout[0, d] = stage_u[ring, d].astype(jnp.bfloat16)
        tiles_loop(conv)
        store_piece(outs7, me, s * N, cout.at[0], l_so.at[0])

    def convert(slot, seg, chunk):
        pltpu.make_async_copy(at(0, 0), cin.at[slot - 1], l_c.at[slot - 1]).wait()

        def conv(d):
            cout[slot, d] = cin[slot - 1, d].astype(jnp.bfloat16)
        tiles_loop(conv)
        store_piece(outs7, seg, chunk * N, cout.at[slot], l_so.at[slot])

    def fetch(slot, seg, chunk):
        pltpu.make_async_copy(at(seg, chunk), cin.at[slot - 1], l_c.at[slot - 1]).start()

    def stored(slot):
        pltpu.make_async_copy(cout.at[slot], o_wq.at[pl.ds(0, N)], l_so.at[slot]).wait()

    def gather_step(s, carry):
        j = s - 16
        pl.when(s == 2)(state_tail)
        q = s - LAG
        q2 = s - LAG - 1

        @pl.when((s >= 1) & (s <= 16))
        def _():
            stored(0)

        @pl.when(s < 16)
        def _():
            own(s)

        @pl.when((s >= 16) & (s < 24))
        def _():
            remote(at(xn, j), at(xn, j), f_y.at[j], ru_y.at[s], yn).start()
            remote(at(yn, 8 + j), at(yn, 8 + j), f_x.at[j], ru_x.at[s], xn).start()

        @pl.when((q >= 1) & (q <= 24))
        def _():
            stored(1)
            stored(2)

        @pl.when((q2 >= 1) & (q2 <= 24))
        def _():
            stored(3)
            stored(4)

        @pl.when((q2 >= 1) & (q2 <= 16))
        def _():
            stored(5)

        xseg, xc = link_piece(q, 0)
        yseg, yc = link_piece(q, 1)
        par = lax.rem(s, 2)

        @pl.when((q >= 0) & (q < 24))
        def _():
            remote(at(xseg, xc), at(xseg, xc), d_x.at[par], ru_x.at[q], xn).wait_recv()
            copy = remote(at(xseg, xc), at(xseg, xc), d_x.at[par], r_px.at[q], partner)
            pl.when(q >= 2)(copy.wait_send)
            copy.start()
            fetch(1, xseg, xc)
            remote(at(yseg, yc), at(yseg, yc), d_y.at[par], ru_y.at[q], yn).wait_recv()
            copy = remote(at(yseg, yc), at(yseg, yc), d_y.at[par], r_py.at[q], partner)
            pl.when(q >= 2)(copy.wait_send)
            copy.start()
            fetch(2, yseg, yc)

        pxseg, pxc = link_piece(q2, 0)
        pyseg, pyc = link_piece(q2, 1)

        @pl.when((q2 >= 0) & (q2 < 16))
        def _():
            remote(at(partner, q2), at(partner, q2), su_p.at[0], ru_o.at[q2], partner).wait_recv()
            fetch(5, partner, q2)

        @pl.when((q2 >= 0) & (q2 < 24))
        def _():
            remote(at(0, 0), at(0, 0), d_x.at[par], r_px.at[q2], partner).wait_recv()
            fetch(3, pxseg + flip, pxc)
            remote(at(0, 0), at(0, 0), d_y.at[par], r_py.at[q2], partner).wait_recv()
            fetch(4, pyseg + flip, pyc)

        @pl.when((q >= 0) & (q < 24))
        def _():
            convert(1, xseg, xc)
            convert(2, yseg, yc)

        @pl.when((q2 >= 0) & (q2 < 16))
        def _():
            convert(5, partner, q2)

        @pl.when((q2 >= 0) & (q2 < 24))
        def _():
            convert(3, pxseg + flip, pxc)
            convert(4, pyseg + flip, pyc)
        return carry

    lax.fori_loop(0, 24 + LAG + 1, gather_step, 0)
    gains_finish()
    stored(3)
    stored(4)
    for a in range(3):
        pltpu.make_async_copy(st.at[a], outs[a].at[pl.ds(0, ROWS)], l_out.at[a]).wait()
    for ring in range(RING):
        remote(stage_u.at[ring], at(me, 0), su_x.at[ring], ru_x.at[0], xn).wait_send()
        remote(stage_u.at[ring], at(me, 0), su_y.at[ring], ru_y.at[0], yn).wait_send()
        remote(stage_u.at[ring], at(me, 0), su_p.at[ring], ru_o.at[0], partner).wait_send()
    for j in range(HALF):
        remote(at(0, 0), at(0, 0), f_y.at[j], ru_y.at[0], yn).wait_send()
        remote(at(0, 0), at(0, 0), f_x.at[j], ru_x.at[0], xn).wait_send()
    for par in (0, 1):
        remote(at(0, 0), at(0, 0), d_x.at[par], r_px.at[0], partner).wait_send()
        remote(at(0, 0), at(0, 0), d_y.at[par], r_py.at[0], partner).wait_send()


ANY = pl.BlockSpec(memory_space=pl.ANY)
VMEM = pl.BlockSpec(memory_space=pltpu.VMEM)
SMEM = pl.BlockSpec(memory_space=pltpu.SMEM)
F32 = jnp.float32
BF16 = jnp.bfloat16
LIMIT = 62 * 1024 * 1024


def to_tiles(x):
    rows, cols = x.shape[-2:]
    lead = x.size // cols
    return x.reshape(lead // 8, 8, cols // LANES, LANES).transpose(0, 2, 1, 3).reshape(-1, 8, LANES)


def from_tiles(t, shape):
    cols = shape[-1]
    lead = t.size // cols
    return t.reshape(lead // 8, cols // LANES, 8, LANES).transpose(0, 2, 1, 3).reshape(shape)


def local_step(*arrays):
    grads = arrays[:10]
    states = [a.reshape(LOCAL_ROWS, LANES) for a in arrays[10:13]]
    dma = pltpu.SemaphoreType.DMA
    chunk = (N, 8, LANES)
    shape = jax.ShapeDtypeStruct
    flat = shape((LOCAL_ROWS, LANES), F32)
    tile_counts = (2592, 864, 864, 2592, 6912, 6912, 6912)
    vm = pltpu.VMEM
    res = pl.pallas_call(
        step_kernel,
        out_shape=[flat] * 3 + [shape((c, 8, LANES), BF16) for c in tile_counts]
        + [shape((2, 1152), BF16), shape((2, 1152), BF16), shape((1, 1152), BF16), shape((8, LANES), F32),
           shape((SEG_ROWS + TAIL, LANES), F32), shape((24,) + chunk, F32), shape((24,) + chunk, F32),
           shape((64,) + chunk, F32), shape((8, SEG_TILES, 8, LANES), F32)],
        in_specs=[ANY] * 7 + [VMEM] * 3 + [ANY] * 3 + [SMEM],
        out_specs=[ANY] * 10 + [VMEM] * 4 + [ANY] * 5,
        scratch_shapes=[vm((2,) + chunk, BF16), vm((2,) + chunk, BF16), vm((2,) + chunk, BF16),
                        vm((2,) + chunk, F32), vm((2,) + chunk, F32), vm((3, 2) + chunk, F32),
                        vm((RING, 2) + chunk, F32), vm((2, 3) + chunk, F32), vm((2, ROWS, LANES), F32),
                        vm((3, 8, LANES), F32), vm((3, 8, LANES), F32), vm((8, LANES), F32),
                        vm((7, 24, 8, LANES), BF16), vm((8, 192, LANES), F32), vm((7, TAIL, LANES), F32), vm((TAIL, LANES), F32),
                        vm((3, 56, LANES), F32), vm((3, 104, LANES), F32), vm((104, LANES), F32), vm((56, LANES), F32), vm((56, LANES), F32), vm((8, LANES), F32),
                        vm((ROWS + TAIL, LANES), F32), vm((3, ROWS, LANES), F32), vm((ROWS + TAIL, LANES), F32),
                        vm((RING,) + chunk, F32), vm((5,) + chunk, F32), vm((6,) + chunk, BF16),
                        dma((RING,)), dma((RING,)), dma((3, 2)), dma((24,)), dma((24,)), dma((64,)),
                        dma((2,)), dma((2,)), dma((2,)), dma((2,)), dma((2,)), dma((2, 3)), dma((2,)), dma((3,)), dma((3,)),
                        dma((7,)), dma((7,)), dma((7,)), dma((6,)), dma, dma, dma, dma((3,)), dma((7,)), dma,
                        dma((RING,)), dma((RING,)), dma((RING,)), dma((24,)), dma((24,)), dma((16,)), dma((24,)), dma((24,)),
                        dma((HALF,)), dma((HALF,)), dma((2,)), dma((2,)), dma((4,)), dma((3,)), dma((5,)), dma((6,))],
        compiler_params=pltpu.CompilerParams(collective_id=0, has_side_effects=True, vmem_limit_bytes=LIMIT),
        name="adamw_step",
    )(*[to_tiles(x) for x in grads[:7]], *grads[7:], *states, arrays[13].reshape(1))
    params = [from_tiles(t, x.shape[1:]) for t, x in zip(res[3:10], grads[:7])]
    return tuple([a.reshape(-1) for a in res[:3]] + params + [res[10], res[11], res[12].reshape(-1), res[13][0, 0]])


def solution(mesh):
    return jax.shard_map(local_step, mesh=mesh, in_specs=(P("dp"),) * 13 + (P(),), out_specs=(P("dp"),) * 3 + (P(),) * 11, check_vma=False)
```

```python
import functools
import jax
import jax.numpy as jnp
from jax import lax
from jax.experimental import pallas as pl
from jax.experimental.pallas import tpu as pltpu
from jax.sharding import PartitionSpec as P

BETA_ONE = 0.9
BETA_TWO = 0.95
ADAM_EPS = 1e-8
WEIGHT_DECAY = 0.1
MAX_NORM = 1.0
CLIP_EPS = 1e-6
STEP = 4
BIAS_ONE = 1.0 - BETA_ONE ** STEP
BIAS_TWO = 1.0 - BETA_TWO ** STEP

MESH = pl.DeviceIdType.MESH
F32 = jnp.float32
BF16 = jnp.bfloat16
LANES = 128
SEG_TILES = 3456
SEG_ROWS = SEG_TILES * 8
LOCAL_ROWS = SEG_ROWS + 6
MATRIX_ROWS = 8 * SEG_ROWS
TAIL = 48
WIN = 27600
N = 216
ROWS = N * 8
HALF = SEG_TILES // 2 // N
BOTH = 2 * HALF
SLOTS = 3 * HALF
LATE = 3
RING = 4
LAG = 5
COUNTS = (2592, 864, 864, 2592, 6912, 6912, 6912)
FRONT = ((2, 0, 6, 3),) + tuple((k, t, 24, 24) for k in (4, 5) for t in (0, SEG_TILES)) + tuple((6, t, 9, 9) for t in (0, SEG_TILES))
LIMIT = 62 * 1024 * 1024


def neighbours(me):
    core = lax.rem(me, 2)
    x = lax.rem(lax.div(me, 2), 2)
    y = lax.div(me, 4)
    flip = 1 - 2 * core
    xn = me + 2 - 4 * x
    yn = me + 4 - 8 * y
    diag = xn + 4 - 8 * y
    return flip, me + flip, xn, yn, diag


def on_piece(refs, seg, tile, act):
    wq, wk, wv, wo, gate, up, down = refs
    pl.when((seg == 0) & (tile < 2592))(lambda: act(wq, tile))
    pl.when((seg == 0) & (tile >= 2592))(lambda: act(wk, tile - 2592))
    pl.when((seg == 1) & (tile < 864))(lambda: act(wv, tile))
    pl.when((seg == 1) & (tile >= 864))(lambda: act(wo, tile - 864))
    pl.when((seg == 2) | (seg == 3))(lambda: act(gate, (seg - 2) * SEG_TILES + tile))
    pl.when((seg == 4) | (seg == 5))(lambda: act(up, (seg - 4) * SEG_TILES + tile))
    pl.when((seg == 6) | (seg == 7))(lambda: act(down, (seg - 6) * SEG_TILES + tile))


def on_width(seg, tile, act):
    narrow = ((seg == 0) & (tile >= 2592)) | ((seg == 1) & (tile < 864))
    wide = (seg >= 2) & (seg < 6)
    pl.when(wide)(lambda: act(24))
    pl.when(narrow)(lambda: act(3))
    pl.when(jnp.logical_not(wide | narrow))(lambda: act(9))


def load_piece(refs, seg, tile, buf, sem):
    def act(ref, off):
        pltpu.make_async_copy(ref.at[pl.ds(off, N)], buf, sem).start()
    on_piece(refs, seg, tile, act)


def store_piece(refs, seg, tile, buf, sem):
    def act(ref, off):
        pltpu.make_async_copy(buf, ref.at[pl.ds(off, N)], sem).start()
    on_piece(refs, seg, tile, act)


def tiles_loop(body, group=12):
    def step(i, carry):
        body(pl.ds(pl.multiple_of(i * group, group), group))
        return carry
    lax.fori_loop(0, N // group, step, 0)


def remote(src, dst, send, recv, dev):
    return pltpu.make_async_remote_copy(src_ref=src, dst_ref=dst, send_sem=send, recv_sem=recv, device_id=(dev,), device_id_type=MESH)


def greet(devs):
    barrier = pltpu.get_barrier_semaphore()
    for dev in devs:
        pl.semaphore_signal(barrier, inc=1, device_id=(dev,), device_id_type=MESH)
    pl.semaphore_wait(barrier, len(devs))


def adam(g, p, m, v, lr, decay):
    m = BETA_ONE * m + (1.0 - BETA_ONE) * g
    v = BETA_TWO * v + (1.0 - BETA_TWO) * g * g
    direction = (m * (1.0 / BIAS_ONE)) / (jnp.sqrt(v * (1.0 / BIAS_TWO)) + ADAM_EPS)
    return p - lr * (decay * p + direction), m, v


def local(src, dst, sem):
    return pltpu.make_async_copy(src, dst, sem)


def step_kernel(*args):
    refs, small, ins, rate = args[:7], args[7:10], args[10:13], args[13]
    outs, outs7, gains_out, o_norm = args[14:17], args[17:24], args[24:27], args[27]
    g_flat, land_l, land_p, land, spare_x, spare_y = args[28:34]
    (raw, stage_p, stage_u, aux, stage, own_in, own_g, norm_send, norm_land, n_out, front_raw, front, front_land, tail_g,
     window, halo, window_g, gains_send, gains_land, gb, st, pb, cin, cout) = args[34:58]
    (s_l, s_p, r_l, r_p, l_raw, l_aux, l_own, l_g, s_n, r_n, l_front, s_front, r_front, l_win, s_win, r_win, l_tail, l_six, s_gain, r_gain,
     su, ru, ru_o, r_d, s_f, s_d, l_in, l_out, l_c, l_so) = args[58:]
    spare = (spare_x, spare_y)
    me = lax.axis_index("dp")
    flip, partner, xn, yn, diag = neighbours(me)
    links = (xn, yn)
    pair = range(len(links))
    trio = range(len(ins))
    others = [lax.rem(me + o, 8) for o in range(1, 8)]
    shift = 6 * me
    lr = rate[0]
    n_out[...] = jnp.zeros_like(n_out)
    window[...] = jnp.zeros_like(window)
    window_g[...] = jnp.zeros_like(window_g)
    halo[:, pl.ds(56, TAIL), :] = jnp.zeros((3, TAIL, LANES), F32)
    front[7] = jnp.zeros(front.shape[1:], F32)
    greet(others)

    def raw_wait(kind, a):
        local(refs[0].at[pl.ds(0, N)], raw.at[kind, a], l_raw.at[kind, a]).wait()

    def to_partner(par, a, slot):
        return remote(stage_p.at[par, a], land_p.at[slot], s_p.at[par, a], r_p.at[slot], partner)

    def to_link(ring, a, slot):
        return remote(stage.at[ring, a], land_l.at[a, slot], s_l.at[ring, a], r_l.at[a, slot], links[a])

    def window_copies():
        out = []
        for a in trio:
            for row, place, rows in ((WIN, 0, TAIL), (SEG_ROWS, TAIL, 6)):
                out.append(local(ins[a].at[pl.ds(row, rows)], window.at[a, pl.ds(place, rows)], l_win.at[len(out)]))
        return out

    def front_copies():
        return [local(refs[k].at[pl.ds(off, cnt)], front_raw.at[d, pl.ds(0, cnt)], l_front.at[d]) for d, (k, off, cnt, width) in enumerate(FRONT)]

    def front_sends():
        return [remote(front.at[dev, pl.ds(0, TAIL)], front_land.at[o], s_front.at[o], r_front.at[o], dev) for o, dev in enumerate(others)]

    def window_send():
        return remote(window, halo.at[:, pl.ds(0, 56)], s_win, r_win, others[0])

    def small_exchange():
        for copy in window_copies() + front_copies():
            copy.start()
        place = 0
        for ref, count in zip(small, (2, 2, 1)):
            value = ref[...].reshape(count, 9 * LANES).astype(F32)
            for r in range(count):
                for w in range(9):
                    front[7, pl.ds(place, 1), :] = value[r:r + 1, w * LANES:(w + 1) * LANES]
                    place += 1
        for copy in window_copies() + front_copies():
            copy.wait()
        for d, (k, off, cnt, width) in enumerate(FRONT):
            for t in range(cnt):
                front[d, pl.ds(t // width * 8 * width + t % width, 8, stride=width), :] = front_raw[d, t].astype(F32)
        window_send().start()
        for copy in front_sends():
            copy.start()

    def small_finish():
        total = front[me, pl.ds(0, TAIL), :]
        for o, copy in enumerate(front_sends()):
            copy.wait()
            total = total + front_land[o]
        window_send().wait()
        total = total * 0.125
        tail_g[...] = total

        @pl.when(me == 7)
        def _():
            n_out[...] += jnp.sum((total * total).reshape(TAIL // 8, 8, LANES), axis=0)
        copy = local(tail_g, g_flat.at[pl.ds(SEG_ROWS, TAIL)], l_tail)
        copy.start()
        copy.wait()

    def link_jobs(s):
        jobs = []
        for a in pair:
            half = jnp.where(s < BOTH, a, 1 - a)
            seg = jnp.where(s < HALF, diag, links[a])
            jobs.append((seg, (half * HALF + lax.rem(s, HALF)) * N, a * SLOTS + s))
        return jobs

    def own_jobs(j):
        return [(me, (h * HALF + j) * N, 2 * SLOTS + h * HALF + j) for h in pair]

    def give(jobs, kind, par, wait_old):
        for a, (seg, tile, slot) in enumerate(jobs):
            load_piece(refs, seg + flip, tile, raw.at[kind, a], l_raw.at[kind, a])
        for a, (seg, tile, slot) in enumerate(jobs):
            raw_wait(kind, a)
            copy = to_partner(par, a, slot)
            pl.when(wait_old)(copy.wait_send)

            def conv(d, a=a):
                stage_p[par, a, d] = raw[kind, a, d].astype(F32)
            tiles_loop(conv)
            copy.start()

    def step(s, count):
        j = lax.rem(s, HALF)
        ring = lax.rem(s, RING)

        @pl.when(s < SLOTS - 1)
        def _():
            give(link_jobs(s + 1), 0, lax.rem(s + 1, 2), s >= 1)

        @pl.when(s < SLOTS)
        def _():
            jobs = link_jobs(s)
            for a, (seg, tile, slot) in enumerate(jobs):
                load_piece(refs, seg, tile, raw.at[1, a], l_raw.at[1, a])
            for a, (seg, tile, slot) in enumerate(jobs):
                to_partner(0, a, slot).wait_recv()
                local(land_p.at[slot], aux.at[0, a], l_aux.at[0, a]).start()

            @pl.when(s >= BOTH)
            def _():
                for a in pair:
                    to_link(0, a, j).wait_recv()
                for a in pair:
                    local(land_l.at[1 - a, j], aux.at[1, a], l_aux.at[1, a]).start()
            for a in pair:
                raw_wait(1, a)
                local(land_p.at[0], aux.at[0, a], l_aux.at[0, a]).wait()
                copy = to_link(ring, a, s)
                pl.when(s >= RING)(copy.wait_send)

                @pl.when(s < BOTH)
                def _(a=a):
                    def add(d):
                        stage[ring, a, d] = raw[1, a, d].astype(F32) + aux[0, a, d]
                    tiles_loop(add)

                @pl.when(s >= BOTH)
                def _(a=a):
                    local(land_p.at[0], aux.at[1, a], l_aux.at[1, a]).wait()

                    def add(d):
                        stage[ring, a, d] = raw[1, a, d].astype(F32) + aux[0, a, d] + aux[1, a, d]
                    tiles_loop(add)
                copy.start()

        pl.when(s == 2)(small_exchange)
        pl.when(s == BOTH + 4)(small_finish)

        @pl.when((s >= HALF + 4) & (s < BOTH + 4))
        def _():
            give(own_jobs(s - HALF - 4), 2, 2, s > HALF + 4)

        @pl.when(s >= BOTH + LAG)
        def _():
            take_own(s - BOTH - LAG)
        return count

    def take_own(j):
        for h, (seg, tile, slot) in enumerate(own_jobs(j)):
            load_piece(refs, seg, tile, raw.at[2, h], l_raw.at[2, h])
            to_partner(2, h, slot).wait_recv()
            local(land_p.at[slot], own_in.at[h, 0], l_own.at[h, 0]).start()
        for k in (1, 2):
            for h in pair:
                a = h if k == 1 else 1 - h
                slot = k * HALF + j
                to_link(0, a, slot).wait_recv()
                local(land_l.at[a, slot], own_in.at[h, k], l_own.at[h, k]).start()
        for h, (seg, tile, slot) in enumerate(own_jobs(j)):
            raw_wait(2, h)
            for a in trio:
                local(land_p.at[0], own_in.at[h, a], l_own.at[h, a]).wait()
            row = pl.multiple_of(tile * 8, 8)
            out = local(own_g.at[h], g_flat.at[pl.ds(row, ROWS)], l_g.at[h])
            pl.when(j >= 1)(out.wait)

            def relay(width, h=h):
                def body(r, acc):
                    for w in range(width):
                        t = r * width + w
                        g = (raw[2, h, t].astype(F32) + own_in[h, 0, t] + own_in[h, 1, t] + own_in[h, 2, t]) * 0.125
                        own_g[h, pl.ds(r * (8 * width) + w, 8, stride=width), :] = g
                        acc = acc + g * g
                    return acc
                n_out[...] += lax.fori_loop(0, N // width, body, jnp.zeros((8, LANES), F32))
            on_width(me, tile, relay)
            out.start()

    def state_loads(s):
        row = pl.multiple_of(s * ROWS, 8)
        for a in trio:
            local(ins[a].at[pl.ds(row, ROWS)], st.at[a], l_in.at[a]).start()

    def gradient_load(s):
        row = pl.multiple_of(s * ROWS, 8)
        return local(g_flat.at[pl.ds(row, ROWS + TAIL)], gb, l_in.at[3])

    give(link_jobs(0), 0, 0, False)
    lax.fori_loop(0, SLOTS + LAG, step, 0)
    state_loads(0)

    for r, dev in enumerate((partner, xn, yn)):
        norm_send[r] = n_out[...]
        copy = remote(norm_send.at[r], norm_land.at[r], s_n.at[r], r_n.at[r], dev)
        copy.start()
        copy.wait()
        n_out[...] += norm_land[r]
    for h in pair:
        local(own_g.at[h], g_flat.at[pl.ds(0, ROWS)], l_g.at[h]).wait()
    gradient_load(0).start()
    norm = jnp.sqrt(jnp.sum(n_out[...], axis=(0, 1), keepdims=True))
    o_norm[...] = jnp.broadcast_to(norm, (8, LANES))
    n_out[...] = jnp.broadcast_to(jnp.minimum(1.0, MAX_NORM / (norm + CLIP_EPS)), (8, LANES))
    coef = n_out[pl.ds(0, 1), :]
    for a in pair:
        for par in trio:
            to_partner(par, a, 0).wait_send()
        for ring in range(RING):
            to_link(ring, a, 0).wait_send()

    def state_tail():
        copy = local(g_flat.at[pl.ds(WIN, 2 * TAIL)], window_g.at[pl.ds(0, 2 * TAIL)], l_tail)
        copy.start()
        copy.wait()
        place = lax.broadcasted_iota(jnp.int32, (56, LANES), 0) + (me * LOCAL_ROWS + WIN)
        decay = jnp.where(place < MATRIX_ROWS, WEIGHT_DECAY, 0.0)
        new = adam(window_g[pl.ds(shift, 56), :] * coef, window[0], window[1], window[2], lr, decay)
        gains_send[...] = new[0]
        for a in trio:
            window[a] = new[a]
            six_store(a).start()

        @pl.when(me == 7)
        def _():
            for o, dev in enumerate(others):
                gains_copy(o, dev).start()

    def six_store(a):
        return local(window.at[a, pl.ds(TAIL, 6)], outs[a].at[pl.ds(SEG_ROWS, 6)], l_six.at[a])

    def gains_copy(o, dev):
        return remote(gains_send, gains_land, s_gain.at[o], r_gain, dev)

    def gains_finish():
        def write(src):
            t = src[...]

            def row(r):
                return jnp.concatenate([t[6 + 9 * r + w:7 + 9 * r + w, :] for w in range(9)], axis=1)
            for out, rows in zip(gains_out, ((0, 1), (2, 3), (4,))):
                out[...] = jnp.concatenate([row(r) for r in rows], axis=0).astype(BF16)

        @pl.when(me == 7)
        def _():
            for o, dev in enumerate(others):
                gains_copy(o, dev).wait_send()
            write(gains_send)

        @pl.when(me != 7)
        def _():
            gains_copy(0, others[0]).wait_recv()
            write(gains_land)
        for a in trio:
            six_store(a).wait()

    def first_rows():
        part = pl.ds(54 - shift, TAIL)
        pb[pl.ds(0, TAIL), :] = adam(gb[pl.ds(0, TAIL), :] * coef, halo[0, part, :], halo[1, part, :], halo[2, part, :], lr, WEIGHT_DECAY)[0]

    def at(seg, c):
        return land.at[seg, pl.ds(pl.multiple_of(c * N, N), N)]

    def place(a, seg, chunk, q, act):
        low = (1 + a) * HALF - LATE
        late = (q >= low) & (q < low + LATE)
        pl.when(late)(lambda: act(spare[a].at[pl.ds((q - low) * N, N)]))
        pl.when(jnp.logical_not(late))(lambda: act(at(seg, chunk)))

    def link_piece(q, a):
        direct = q < BOTH
        return jnp.where(direct, links[a], diag), jnp.where(direct, q, q - (1 + a) * HALF)

    def own(s):
        ring = lax.rem(s, RING)
        row = pl.multiple_of(s * ROWS, 8)

        def state_store(a):
            return local(st.at[a], outs[a].at[pl.ds(row, ROWS)], l_out.at[a])

        @pl.when(s >= 1)
        def _():
            gradient_load(s).start()
            for a in trio:
                state_store(a).wait()
            state_loads(s)
        gradient_load(s).wait()
        for a in trio:
            local(ins[a].at[pl.ds(row, ROWS)], st.at[a], l_in.at[a]).wait()
        pl.when(s == 0)(first_rows)
        slab = 48
        base = me * LOCAL_ROWS + s * ROWS

        def update(i, carry):
            d = pl.ds(pl.multiple_of(i * slab, 8), slab)
            e = pl.ds(i * slab + shift, slab)
            rows = lax.broadcasted_iota(jnp.int32, (slab, LANES), 0) + (base + i * slab)
            decay = jnp.where(rows < MATRIX_ROWS, WEIGHT_DECAY, 0.0)
            new = adam(gb[e, :] * coef, st[0, d, :], st[1, d, :], st[2, d, :], lr, decay)
            for a in trio:
                st[a, d, :] = new[a]
            pb[e, :] = new[0]
            return carry
        lax.fori_loop(0, ROWS // slab, update, 0)
        for a in trio:
            state_store(a).start()
        devs = links + (partner,)

        @pl.when(s >= RING)
        def _():
            for a in trio:
                remote(stage_u.at[ring], at(me, s), su.at[a, ring], ru_o.at[s], devs[a]).wait_send()

        def relay(width):
            def body(r, carry):
                for w in range(width):
                    stage_u[ring, r * width + w] = pb[pl.ds(r * (8 * width) + w, 8, stride=width), :]
                return carry
            lax.fori_loop(0, N // width, body, 0)
        on_width(me, s * N, relay)
        pb[pl.ds(0, TAIL), :] = pb[pl.ds(ROWS, TAIL), :]
        for a in pair:
            place(a, me, s, s, lambda ref, a=a: remote(stage_u.at[ring], ref, su.at[a, ring], ru.at[a, s], devs[a]).start())
        remote(stage_u.at[ring], at(me, s), su.at[2, ring], ru_o.at[s], partner).start()

        def conv(d):
            cout[5, d] = stage_u[ring, d].astype(BF16)
        tiles_loop(conv)
        store_piece(outs7, me, s * N, cout.at[5], l_so.at[5])

    def convert(k, seg, chunk):
        local(at(0, 0), cin.at[k], l_c.at[k]).wait()

        def conv(d):
            cout[k, d] = cin[k, d].astype(BF16)
        tiles_loop(conv)
        store_piece(outs7, seg, chunk * N, cout.at[k], l_so.at[k])

    def fetch(k, ref):
        local(ref, cin.at[k], l_c.at[k]).start()

    def stored(k):
        local(cout.at[k], outs7[0].at[pl.ds(0, N)], l_so.at[k]).wait()

    last = SLOTS - LATE

    def link_wait(a, q):
        return remote(at(0, 0), at(0, 0), s_d.at[a, 0], ru.at[a, q], links[a])

    def hand(a, par, q, src, dst):
        return remote(src, dst, s_d.at[a, par], r_d.at[a, q], partner)

    def forward(a, seg, chunk, j):
        return remote(at(seg, chunk), at(seg, chunk), s_f.at[a, j], ru.at[a, BOTH + j], links[a])

    def gather_step(s, carry):
        j = s - BOTH
        q = s - LAG
        z = q - 1
        par = lax.rem(s, 2)
        arrives = (q >= 0) & (q < last)
        from_partner = (z >= 0) & (z < last)
        own_partner = (z >= 0) & (z < BOTH)
        pl.when(s == 2)(state_tail)
        pl.when((s >= 1) & (s <= BOTH))(lambda: stored(5))
        pl.when(s < BOTH)(lambda: own(s))

        @pl.when((j >= 0) & (j < HALF - LATE))
        def _():
            forward(1, xn, j, j).start()
            forward(0, yn, HALF + j, j).start()

        @pl.when((q >= 1) & (q <= last))
        def _():
            for a in pair:
                stored(a)

        @pl.when((z >= 1) & (z <= last))
        def _():
            for a in pair:
                stored(2 + a)

        pl.when((z >= 1) & (z <= BOTH))(lambda: stored(4))

        @pl.when(arrives)
        def _():
            for a in pair:
                seg, chunk = link_piece(q, a)
                link_wait(a, q).wait_recv()
                pl.when(q >= 2)(hand(a, par, q, at(0, 0), at(0, 0)).wait_send)

                def act(ref, a=a, seg=seg, chunk=chunk):
                    hand(a, par, q, ref, at(seg, chunk)).start()
                    fetch(a, ref)
                place(a, seg, chunk, q, act)

        @pl.when(own_partner)
        def _():
            remote(at(0, 0), at(0, 0), su.at[2, 0], ru_o.at[z], partner).wait_recv()
            fetch(4, at(partner, z))

        @pl.when(from_partner)
        def _():
            for a in pair:
                seg, chunk = link_piece(z, a)
                hand(a, 0, z, at(0, 0), at(0, 0)).wait_recv()
                fetch(2 + a, at(seg + flip, chunk))

        @pl.when(arrives)
        def _():
            for a in pair:
                convert(a, *link_piece(q, a))

        pl.when(own_partner)(lambda: convert(4, partner, z))

        @pl.when(from_partner)
        def _():
            for a in pair:
                seg, chunk = link_piece(z, a)
                convert(2 + a, seg + flip, chunk)
        return carry

    lax.fori_loop(0, last + LAG + 1, gather_step, 0)
    gains_finish()
    for a in pair:
        stored(2 + a)
        for par in pair:
            hand(a, par, 0, at(0, 0), at(0, 0)).wait_send()
        for j in range(HALF - LATE):
            forward(a, 0, 0, j).wait_send()
    for a in trio:
        local(st.at[a], outs[a].at[pl.ds(0, ROWS)], l_out.at[a]).wait()
        for ring in range(RING):
            remote(stage_u.at[ring], at(me, 0), su.at[a, ring], ru_o.at[0], partner).wait_send()


def copy_kernel(*args):
    ins, outs, (wide, thin, l_in, l_out) = args[:10], args[10:20], args[20:]
    depth = wide.shape[0]
    jobs = []
    for src, dst in zip(ins, outs):
        size, kind = src.shape[0], len(src.shape) - 2
        piece = (SEG_ROWS // 8, COUNTS[1])[kind]
        for off in range(0, size, piece):
            rows = pl.ds(off, min(piece, size - off))
            n = len(jobs)
            buf = (wide, thin)[kind].at[n % depth, pl.ds(0, rows.size)]
            jobs.append((local(src.at[rows], buf, l_in.at[n % depth]), local(buf, dst.at[rows], l_out.at[n % depth])))
    ahead = depth // 2
    for n in range(len(jobs) + ahead):
        if n < len(jobs):
            if n >= depth:
                jobs[n - depth][1].wait()
            jobs[n][0].start()
        if n >= ahead:
            jobs[n - ahead][0].wait()
            jobs[n - ahead][1].start()
    for job in jobs[-depth:]:
        job[1].wait()


def late_kernel(mine, *args):
    came, outs7 = args[:2], args[9:16]
    cin, cout, l_in, l_out = args[16:]
    flip, partner, xn, yn, diag = neighbours(lax.axis_index("dp"))
    seg = diag if mine else diag + flip
    jobs = [(a, i, a * LATE + i) for a in range(2) for i in range(LATE)]
    loads = [local(came[a].at[pl.ds(i * N, N)], cin.at[k], l_in.at[k]) for a, i, k in jobs]
    for load in loads:
        load.start()
    for a, i, k in jobs:
        loads[k].wait()

        def conv(d, k=k):
            cout[k, d] = cin[k, d].astype(BF16)
        tiles_loop(conv)
        store_piece(outs7, seg, ((1 + a) * HALF - LATE + i) * N + 0 * seg, cout.at[k], l_out.at[k])
    for k in range(2 * LATE):
        local(cout.at[k], outs7[0].at[pl.ds(0, N)], l_out.at[k]).wait()


ANY = pl.BlockSpec(memory_space=pl.ANY)
VMEM = pl.BlockSpec(memory_space=pltpu.VMEM)
SMEM = pl.BlockSpec(memory_space=pltpu.SMEM)


def to_tiles(x):
    cols = x.shape[-1]
    lead = x.size // cols
    return x.reshape(lead // 8, 8, cols // LANES, LANES).transpose(0, 2, 1, 3).reshape(-1, 8, LANES)


def from_tiles(t, shape):
    cols = shape[-1]
    lead = t.size // cols
    return t.reshape(lead // 8, cols // LANES, 8, LANES).transpose(0, 2, 1, 3).reshape(shape)


def shapes(kind, dtype, *dims):
    return [kind(d, dtype) for d in dims]


def dmas(*dims):
    return [pltpu.SemaphoreType.DMA(d) if d else pltpu.SemaphoreType.DMA for d in dims]


def params_of(**kw):
    return pltpu.CompilerParams(vmem_limit_bytes=LIMIT, has_side_effects=True, **kw)


def copy_call(arrays):
    depth = 12
    moved = 2 * sum(a.size * a.dtype.itemsize for a in arrays)
    return pl.pallas_call(
        copy_kernel,
        out_shape=[jax.ShapeDtypeStruct(a.shape, a.dtype) for a in arrays],
        in_specs=[ANY] * 10,
        out_specs=[ANY] * 10,
        scratch_shapes=[pltpu.VMEM((depth, SEG_ROWS // 8, LANES), F32), pltpu.VMEM((depth, COUNTS[1], 8, LANES), BF16)] + dmas((depth,), (depth,)),
        compiler_params=params_of(),
        cost_estimate=pl.CostEstimate(flops=100 * moved, bytes_accessed=moved, transcendentals=0),
        name="copy_results",
    )(*arrays)


def late_call(mine, came, tiles):
    chunks = 2 * LATE
    return pl.pallas_call(
        functools.partial(late_kernel, mine),
        out_shape=[jax.ShapeDtypeStruct(a.shape, a.dtype) for a in tiles],
        in_specs=[ANY] * 9,
        out_specs=[ANY] * 7,
        input_output_aliases={2 + k: k for k in range(7)},
        scratch_shapes=[pltpu.VMEM((chunks, N, 8, LANES), F32), pltpu.VMEM((chunks, N, 8, LANES), BF16)] + dmas((chunks,), (chunks,)),
        compiler_params=params_of(),
        cost_estimate=pl.CostEstimate(flops=came[0].size * 1000, bytes_accessed=came[0].size * 12, transcendentals=0),
        name="late_chunks",
    )(*came, *tiles)


def local_step(*arrays):
    grads = arrays[:10]
    states = [a.reshape(LOCAL_ROWS, LANES) for a in arrays[10:13]]
    chunk = (N, 8, LANES)
    sds = jax.ShapeDtypeStruct
    vm = pltpu.VMEM
    deep = len(FRONT)
    late = (LATE * N, 8, LANES)
    two, three, eight, width = 2, 3, 8, 1152
    tile, tail, long = (eight, LANES), (56, LANES), (104, LANES)
    res = pl.pallas_call(
        step_kernel,
        out_shape=shapes(sds, F32, *[(LOCAL_ROWS, LANES)] * three) + shapes(sds, BF16, *[(c, eight, LANES) for c in COUNTS], (two, width), (two, width), (1, width))
        + shapes(sds, F32, (eight, LANES), (SEG_ROWS + TAIL, LANES), (two, SLOTS) + chunk, (2 * SLOTS + BOTH,) + chunk, (eight, SEG_TILES, eight, LANES), late, late),
        in_specs=[ANY] * 7 + [VMEM] * 3 + [ANY] * 3 + [SMEM],
        out_specs=[ANY] * 10 + [VMEM] * 4 + [ANY] * 6,
        scratch_shapes=shapes(vm, BF16, (three, two) + chunk)
        + shapes(vm, F32, (three, two) + chunk, (RING,) + chunk, (two, two) + chunk, (RING, two) + chunk, (two, three) + chunk, (two, ROWS, LANES),
                 (three, *tile), (three, *tile), (eight, LANES))
        + shapes(vm, BF16, (deep, 24, eight, LANES))
        + shapes(vm, F32, (eight, 192, LANES), (deep, TAIL, LANES), (TAIL, LANES), (three, *tail), (three, *long), long, tail, tail,
                 (ROWS + TAIL, LANES), (three, ROWS, LANES), (ROWS + TAIL, LANES), (5,) + chunk)
        + shapes(vm, BF16, (6,) + chunk)
        + dmas((RING, two), (three, two), (two, SLOTS), (2 * SLOTS + BOTH,), (three, two), (two, two), (two, three), (two,), (three,), (three,),
               (deep,), (deep,), (deep,), (6,), None, None, None, (three,), (deep,), None,
               (three, RING), (two, SLOTS), (BOTH,), (two, SLOTS), (two, HALF), (two, two), (4,), (three,), (5,), (6,)),
        compiler_params=params_of(collective_id=0),
        name="adamw_step",
    )(*[to_tiles(x) for x in grads[:7]], *grads[7:], *states, arrays[13].reshape(1))
    kept, (norm, spare_x, spare_y) = res[:10], (res[13], res[18], res[19])

    def swap(x, bit):
        return lax.ppermute(x, "dp", [(i, i ^ bit) for i in range(8)])
    came = (swap(spare_x, 4), swap(spare_y, 2))
    copied = list(copy_call(kept))
    *came, copied[4] = lax.optimization_barrier((*came, copied[4]))
    tiles = late_call(True, came, copied[3:])
    tiles = late_call(False, [swap(c, 1) for c in came], tiles)
    params = [from_tiles(t, x.shape[1:]) for t, x in zip(tiles, grads[:7])]
    return tuple([a.reshape(-1) for a in copied[:3]] + params + [res[10], res[11], res[12].reshape(-1), norm[0, 0]])


def solution(mesh):
    return jax.shard_map(local_step, mesh=mesh, in_specs=(P("dp"),) * 13 + (P(),), out_specs=(P("dp"),) * 3 + (P(),) * 11, check_vma=False)
```

```python
import functools
import jax
import jax.numpy as jnp
from jax import lax
from jax.experimental import pallas as pl
from jax.experimental.pallas import tpu as pltpu
from jax.sharding import PartitionSpec as P

BETA_ONE = 0.9
BETA_TWO = 0.95
ADAM_EPS = 1e-8
WEIGHT_DECAY = 0.1
MAX_NORM = 1.0
CLIP_EPS = 1e-6
STEP = 4
BIAS_ONE = 1.0 - BETA_ONE ** STEP
BIAS_TWO = 1.0 - BETA_TWO ** STEP

MESH = pl.DeviceIdType.MESH
F32 = jnp.float32
BF16 = jnp.bfloat16
LANES = 128
SEG_TILES = 3456
SEG_ROWS = SEG_TILES * 8
LOCAL_ROWS = SEG_ROWS + 6
MATRIX_ROWS = 8 * SEG_ROWS
TAIL = 48
WIN = 27600
N = 144
ROWS = N * 8
HALF = SEG_TILES // 2 // N
BOTH = 2 * HALF
SLOTS = 3 * HALF
LATE = 5
RING = 4
LAG = 5
COUNTS = (2592, 864, 864, 2592, 6912, 6912, 6912)
FRONT = ((2, 0, 6, 3),) + tuple((k, t, 24, 24) for k in (4, 5) for t in (0, SEG_TILES)) + tuple((6, t, 9, 9) for t in (0, SEG_TILES))
LIMIT = 62 * 1024 * 1024


def neighbours(me):
    core = lax.rem(me, 2)
    x = lax.rem(lax.div(me, 2), 2)
    y = lax.div(me, 4)
    flip = 1 - 2 * core
    xn = me + 2 - 4 * x
    yn = me + 4 - 8 * y
    diag = xn + 4 - 8 * y
    return flip, me + flip, xn, yn, diag


def on_piece(refs, seg, tile, act):
    wq, wk, wv, wo, gate, up, down = refs
    pl.when((seg == 0) & (tile < 2592))(lambda: act(wq, tile))
    pl.when((seg == 0) & (tile >= 2592))(lambda: act(wk, tile - 2592))
    pl.when((seg == 1) & (tile < 864))(lambda: act(wv, tile))
    pl.when((seg == 1) & (tile >= 864))(lambda: act(wo, tile - 864))
    pl.when((seg == 2) | (seg == 3))(lambda: act(gate, (seg - 2) * SEG_TILES + tile))
    pl.when((seg == 4) | (seg == 5))(lambda: act(up, (seg - 4) * SEG_TILES + tile))
    pl.when((seg == 6) | (seg == 7))(lambda: act(down, (seg - 6) * SEG_TILES + tile))


def on_width(seg, tile, act):
    narrow = ((seg == 0) & (tile >= 2592)) | ((seg == 1) & (tile < 864))
    wide = (seg >= 2) & (seg < 6)
    pl.when(wide)(lambda: act(24))
    pl.when(narrow)(lambda: act(3))
    pl.when(jnp.logical_not(wide | narrow))(lambda: act(9))


def load_piece(refs, seg, tile, buf, sem):
    def act(ref, off):
        pltpu.make_async_copy(ref.at[pl.ds(off, N)], buf, sem).start()
    on_piece(refs, seg, tile, act)


def store_piece(refs, seg, tile, buf, sem):
    def act(ref, off):
        pltpu.make_async_copy(buf, ref.at[pl.ds(off, N)], sem).start()
    on_piece(refs, seg, tile, act)


def tiles_loop(body, group=12):
    def step(i, carry):
        body(pl.ds(pl.multiple_of(i * group, group), group))
        return carry
    lax.fori_loop(0, N // group, step, 0)


def remote(src, dst, send, recv, dev):
    return pltpu.make_async_remote_copy(src_ref=src, dst_ref=dst, send_sem=send, recv_sem=recv, device_id=(dev,), device_id_type=MESH)


def greet(devs):
    barrier = pltpu.get_barrier_semaphore()
    for dev in devs:
        pl.semaphore_signal(barrier, inc=1, device_id=(dev,), device_id_type=MESH)
    pl.semaphore_wait(barrier, len(devs))


def adam(g, p, m, v, lr, decay):
    m = BETA_ONE * m + (1.0 - BETA_ONE) * g
    v = BETA_TWO * v + (1.0 - BETA_TWO) * g * g
    direction = (m * (1.0 / BIAS_ONE)) / (jnp.sqrt(v * (1.0 / BIAS_TWO)) + ADAM_EPS)
    return p - lr * (decay * p + direction), m, v


def local(src, dst, sem):
    return pltpu.make_async_copy(src, dst, sem)


def step_kernel(*args):
    refs, small, ins, rate = args[:7], args[7:10], args[10:13], args[13]
    outs, outs7, gains_out, o_norm = args[14:17], args[17:24], args[24:27], args[27]
    g_flat, land_l, land_p, land, spare_x, spare_y = args[28:34]
    (raw, stage_p, stage_u, aux, stage, own_in, own_g, norm_send, norm_land, n_out, front_raw, front, front_land, tail_g,
     window, halo, window_g, gains_send, gains_land, gb, st, pb, cin, cout) = args[34:58]
    (s_l, s_p, r_l, r_p, l_raw, l_aux, l_own, l_g, s_n, r_n, l_front, s_front, r_front, l_win, s_win, r_win, l_tail, l_six, s_gain, r_gain,
     su, ru, ru_o, r_d, s_f, s_d, l_in, l_out, l_c, l_so) = args[58:]
    spare = (spare_x, spare_y)
    me = lax.axis_index("dp")
    flip, partner, xn, yn, diag = neighbours(me)
    links = (xn, yn)
    pair = range(len(links))
    trio = range(len(ins))
    others = [lax.rem(me + o, 8) for o in range(1, 8)]
    shift = 6 * me
    lr = rate[0]
    n_out[...] = jnp.zeros_like(n_out)
    window[...] = jnp.zeros_like(window)
    window_g[...] = jnp.zeros_like(window_g)
    halo[:, pl.ds(56, TAIL), :] = jnp.zeros((3, TAIL, LANES), F32)
    front[7] = jnp.zeros(front.shape[1:], F32)

    def raw_wait(kind, a):
        local(refs[0].at[pl.ds(0, N)], raw.at[kind, a], l_raw.at[kind, a]).wait()

    def to_partner(par, a, slot):
        return remote(stage_p.at[par, a], land_p.at[slot], s_p.at[par, a], r_p.at[slot], partner)

    def to_link(ring, a, slot):
        return remote(stage.at[ring, a], land_l.at[a, slot], s_l.at[ring, a], r_l.at[a, slot], links[a])

    def window_copies():
        out = []
        for a in trio:
            for row, place, rows in ((WIN, 0, TAIL), (SEG_ROWS, TAIL, 6)):
                out.append(local(ins[a].at[pl.ds(row, rows)], window.at[a, pl.ds(place, rows)], l_win.at[len(out)]))
        return out

    def front_copies():
        return [local(refs[k].at[pl.ds(off, cnt)], front_raw.at[d, pl.ds(0, cnt)], l_front.at[d]) for d, (k, off, cnt, width) in enumerate(FRONT)]

    def front_sends():
        return [remote(front.at[dev, pl.ds(0, TAIL)], front_land.at[o], s_front.at[o], r_front.at[o], dev) for o, dev in enumerate(others)]

    def window_send():
        return remote(window, halo.at[:, pl.ds(0, 56)], s_win, r_win, others[0])

    def small_exchange():
        for copy in window_copies() + front_copies():
            copy.start()
        place = 0
        for ref, count in zip(small, (2, 2, 1)):
            value = ref[...].reshape(count, 9 * LANES).astype(F32)
            for r in range(count):
                for w in range(9):
                    front[7, pl.ds(place, 1), :] = value[r:r + 1, w * LANES:(w + 1) * LANES]
                    place += 1
        for copy in window_copies() + front_copies():
            copy.wait()
        for d, (k, off, cnt, width) in enumerate(FRONT):
            for t in range(cnt):
                front[d, pl.ds(t // width * 8 * width + t % width, 8, stride=width), :] = front_raw[d, t].astype(F32)
        window_send().start()
        for copy in front_sends():
            copy.start()

    def small_finish():
        total = front[me, pl.ds(0, TAIL), :]
        for o, copy in enumerate(front_sends()):
            copy.wait()
            total = total + front_land[o]
        window_send().wait()
        total = total * 0.125
        tail_g[...] = total

        @pl.when(me == 7)
        def _():
            n_out[...] += jnp.sum((total * total).reshape(TAIL // 8, 8, LANES), axis=0)
        copy = local(tail_g, g_flat.at[pl.ds(SEG_ROWS, TAIL)], l_tail)
        copy.start()
        copy.wait()

    def link_jobs(s):
        jobs = []
        for a in pair:
            half = jnp.where(s < BOTH, a, 1 - a)
            seg = jnp.where(s < HALF, diag, links[a])
            jobs.append((seg, (half * HALF + lax.rem(s, HALF)) * N, a * SLOTS + s))
        return jobs

    def own_jobs(j):
        return [(me, (h * HALF + j) * N, 2 * SLOTS + h * HALF + j) for h in pair]

    def raw_loads(jobs, kind, turn):
        for a, (seg, tile, slot) in enumerate(jobs):
            load_piece(refs, seg + turn, tile, raw.at[kind, a], l_raw.at[kind, a])

    def give(jobs, kind, par, wait_old, load=True):
        if load:
            raw_loads(jobs, kind, flip)
        for a, (seg, tile, slot) in enumerate(jobs):
            raw_wait(kind, a)
            copy = to_partner(par, a, slot)
            pl.when(wait_old)(copy.wait_send)

            def conv(d, a=a):
                stage_p[par, a, d] = raw[kind, a, d].astype(F32)
            tiles_loop(conv)
            copy.start()

    def step(s, count):
        j = lax.rem(s, HALF)
        ring = lax.rem(s, RING)

        @pl.when(s < SLOTS - 1)
        def _():
            give(link_jobs(s + 1), 0, lax.rem(s + 1, 2), s >= 1)

        @pl.when(s < SLOTS)
        def _():
            jobs = link_jobs(s)
            pl.when(s >= 1)(lambda: raw_loads(jobs, 1, 0))
            for a, (seg, tile, slot) in enumerate(jobs):
                to_partner(0, a, slot).wait_recv()
                local(land_p.at[slot], aux.at[0, a], l_aux.at[0, a]).start()

            @pl.when(s >= BOTH)
            def _():
                for a in pair:
                    to_link(0, a, j).wait_recv()
                for a in pair:
                    local(land_l.at[1 - a, j], aux.at[1, a], l_aux.at[1, a]).start()
            for a in pair:
                raw_wait(1, a)
                local(land_p.at[0], aux.at[0, a], l_aux.at[0, a]).wait()
                copy = to_link(ring, a, s)
                pl.when(s >= RING)(copy.wait_send)

                @pl.when(s < BOTH)
                def _(a=a):
                    def add(d):
                        stage[ring, a, d] = raw[1, a, d].astype(F32) + aux[0, a, d]
                    tiles_loop(add)

                @pl.when(s >= BOTH)
                def _(a=a):
                    local(land_p.at[0], aux.at[1, a], l_aux.at[1, a]).wait()

                    def add(d):
                        stage[ring, a, d] = raw[1, a, d].astype(F32) + aux[0, a, d] + aux[1, a, d]
                    tiles_loop(add)
                copy.start()

        pl.when(s == 2)(small_exchange)
        pl.when(s == BOTH + 4)(small_finish)

        @pl.when((s >= HALF + 4) & (s < BOTH + 4))
        def _():
            give(own_jobs(s - HALF - 4), 2, 2, s > HALF + 4)

        @pl.when(s >= BOTH + LAG)
        def _():
            take_own(s - BOTH - LAG)
        return count

    def take_own(j):
        for h, (seg, tile, slot) in enumerate(own_jobs(j)):
            load_piece(refs, seg, tile, raw.at[2, h], l_raw.at[2, h])
            to_partner(2, h, slot).wait_recv()
            local(land_p.at[slot], own_in.at[h, 0], l_own.at[h, 0]).start()
        for k in (1, 2):
            for h in pair:
                a = h if k == 1 else 1 - h
                slot = k * HALF + j
                to_link(0, a, slot).wait_recv()
                local(land_l.at[a, slot], own_in.at[h, k], l_own.at[h, k]).start()
        for h, (seg, tile, slot) in enumerate(own_jobs(j)):
            raw_wait(2, h)
            for a in trio:
                local(land_p.at[0], own_in.at[h, a], l_own.at[h, a]).wait()
            row = pl.multiple_of(tile * 8, 8)
            out = local(own_g.at[h], g_flat.at[pl.ds(row, ROWS)], l_g.at[h])
            pl.when(j >= 1)(out.wait)

            def relay(width, h=h):
                def body(r, acc):
                    for w in range(width):
                        t = r * width + w
                        g = (raw[2, h, t].astype(F32) + own_in[h, 0, t] + own_in[h, 1, t] + own_in[h, 2, t]) * 0.125
                        own_g[h, pl.ds(r * (8 * width) + w, 8, stride=width), :] = g
                        acc = acc + g * g
                    return acc
                n_out[...] += lax.fori_loop(0, N // width, body, jnp.zeros((8, LANES), F32))
            on_width(me, tile, relay)
            out.start()

    def state_loads(s):
        row = pl.multiple_of(s * ROWS, 8)
        for a in trio:
            local(ins[a].at[pl.ds(row, ROWS)], st.at[a], l_in.at[a]).start()

    def gradient_load(s):
        row = pl.multiple_of(s * ROWS, 8)
        return local(g_flat.at[pl.ds(row, ROWS + TAIL)], gb, l_in.at[3])

    raw_loads(link_jobs(0), 0, flip)
    raw_loads(link_jobs(0), 1, 0)
    greet(others)
    give(link_jobs(0), 0, 0, False, False)
    lax.fori_loop(0, SLOTS + LAG, step, 0)
    state_loads(0)

    gradient_load(0).start()

    norm_send[...] = n_out[...]
    norm_land[me] = n_out[...]

    def norm_copy(o, dev, slot):
        return remote(norm_send, norm_land.at[slot], s_n.at[o], r_n.at[slot], dev)
    for o, dev in enumerate(others):
        norm_copy(o, dev, me).start()
    for h in pair:
        local(own_g.at[h], g_flat.at[pl.ds(0, ROWS)], l_g.at[h]).wait()
    for o, dev in enumerate(others):
        norm_copy(o, dev, me).wait_send()
        norm_copy(o, dev, dev).wait_recv()
    n_out[...] = jnp.sum(norm_land[...], axis=0)
    norm = jnp.sqrt(jnp.sum(n_out[...], axis=(0, 1), keepdims=True))
    o_norm[...] = jnp.broadcast_to(norm, (8, LANES))
    n_out[...] = jnp.broadcast_to(jnp.minimum(1.0, MAX_NORM / (norm + CLIP_EPS)), (8, LANES))
    coef = n_out[pl.ds(0, 1), :]
    for a in pair:
        for par in trio:
            to_partner(par, a, 0).wait_send()
        for ring in range(RING):
            to_link(ring, a, 0).wait_send()

    def state_tail():
        copy = local(g_flat.at[pl.ds(WIN, 2 * TAIL)], window_g.at[pl.ds(0, 2 * TAIL)], l_tail)
        copy.start()
        copy.wait()
        place = lax.broadcasted_iota(jnp.int32, (56, LANES), 0) + (me * LOCAL_ROWS + WIN)
        decay = jnp.where(place < MATRIX_ROWS, WEIGHT_DECAY, 0.0)
        new = adam(window_g[pl.ds(shift, 56), :] * coef, window[0], window[1], window[2], lr, decay)
        gains_send[...] = new[0]
        for a in trio:
            window[a] = new[a]
            six_store(a).start()

        @pl.when(me == 7)
        def _():
            for o, dev in enumerate(others):
                gains_copy(o, dev).start()

    def six_store(a):
        return local(window.at[a, pl.ds(TAIL, 6)], outs[a].at[pl.ds(SEG_ROWS, 6)], l_six.at[a])

    def gains_copy(o, dev):
        return remote(gains_send, gains_land, s_gain.at[o], r_gain, dev)

    def gains_finish():
        def write(src):
            t = src[...]

            def row(r):
                return jnp.concatenate([t[6 + 9 * r + w:7 + 9 * r + w, :] for w in range(9)], axis=1)
            for out, rows in zip(gains_out, ((0, 1), (2, 3), (4,))):
                out[...] = jnp.concatenate([row(r) for r in rows], axis=0).astype(BF16)

        @pl.when(me == 7)
        def _():
            for o, dev in enumerate(others):
                gains_copy(o, dev).wait_send()
            write(gains_send)

        @pl.when(me != 7)
        def _():
            gains_copy(0, others[0]).wait_recv()
            write(gains_land)
        for a in trio:
            six_store(a).wait()

    def first_rows():
        part = pl.ds(54 - shift, TAIL)
        pb[pl.ds(0, TAIL), :] = adam(gb[pl.ds(0, TAIL), :] * coef, halo[0, part, :], halo[1, part, :], halo[2, part, :], lr, WEIGHT_DECAY)[0]

    def at(seg, c):
        return land.at[seg, pl.ds(pl.multiple_of(c * N, N), N)]

    def place(a, seg, chunk, q, act):
        low = (1 + a) * HALF - LATE
        late = (q >= low) & (q < low + LATE)
        pl.when(late)(lambda: act(spare[a].at[pl.ds((q - low) * N, N)]))
        pl.when(jnp.logical_not(late))(lambda: act(at(seg, chunk)))

    def link_piece(q, a):
        direct = q < BOTH
        return jnp.where(direct, links[a], diag), jnp.where(direct, q, q - (1 + a) * HALF)

    def own(s):
        ring = lax.rem(s, RING)
        row = pl.multiple_of(s * ROWS, 8)

        def state_store(a):
            return local(st.at[a], outs[a].at[pl.ds(row, ROWS)], l_out.at[a])

        @pl.when(s >= 1)
        def _():
            gradient_load(s).start()
            for a in trio:
                state_store(a).wait()
            state_loads(s)
        gradient_load(s).wait()
        for a in trio:
            local(ins[a].at[pl.ds(row, ROWS)], st.at[a], l_in.at[a]).wait()
        pl.when(s == 0)(first_rows)
        slab = 48
        base = me * LOCAL_ROWS + s * ROWS

        def update(i, carry):
            d = pl.ds(pl.multiple_of(i * slab, 8), slab)
            e = pl.ds(i * slab + shift, slab)
            rows = lax.broadcasted_iota(jnp.int32, (slab, LANES), 0) + (base + i * slab)
            decay = jnp.where(rows < MATRIX_ROWS, WEIGHT_DECAY, 0.0)
            new = adam(gb[e, :] * coef, st[0, d, :], st[1, d, :], st[2, d, :], lr, decay)
            for a in trio:
                st[a, d, :] = new[a]
            pb[e, :] = new[0]
            return carry
        lax.fori_loop(0, ROWS // slab, update, 0)
        for a in trio:
            state_store(a).start()
        devs = links + (partner,)

        @pl.when(s >= RING)
        def _():
            for a in trio:
                remote(stage_u.at[ring], at(me, s), su.at[a, ring], ru_o.at[s], devs[a]).wait_send()

        def relay(width):
            def body(r, carry):
                for w in range(width):
                    stage_u[ring, r * width + w] = pb[pl.ds(r * (8 * width) + w, 8, stride=width), :]
                return carry
            lax.fori_loop(0, N // width, body, 0)
        on_width(me, s * N, relay)
        pb[pl.ds(0, TAIL), :] = pb[pl.ds(ROWS, TAIL), :]
        for a in pair:
            place(a, me, s, s, lambda ref, a=a: remote(stage_u.at[ring], ref, su.at[a, ring], ru.at[a, s], devs[a]).start())
        remote(stage_u.at[ring], at(me, s), su.at[2, ring], ru_o.at[s], partner).start()

        def conv(d):
            cout[5, d] = stage_u[ring, d].astype(BF16)
        tiles_loop(conv)
        store_piece(outs7, me, s * N, cout.at[5], l_so.at[5])

    def convert(k, seg, chunk):
        local(at(0, 0), cin.at[k], l_c.at[k]).wait()

        def conv(d):
            cout[k, d] = cin[k, d].astype(BF16)
        tiles_loop(conv)
        store_piece(outs7, seg, chunk * N, cout.at[k], l_so.at[k])

    def fetch(k, ref):
        local(ref, cin.at[k], l_c.at[k]).start()

    def stored(k):
        local(cout.at[k], outs7[0].at[pl.ds(0, N)], l_so.at[k]).wait()

    last = SLOTS - LATE

    def link_wait(a, q):
        return remote(at(0, 0), at(0, 0), s_d.at[a, 0], ru.at[a, q], links[a])

    def hand(a, par, q, src, dst):
        return remote(src, dst, s_d.at[a, par], r_d.at[a, q], partner)

    def forward(a, seg, chunk, j):
        return remote(at(seg, chunk), at(seg, chunk), s_f.at[a, j], ru.at[a, BOTH + j], links[a])

    def gather_step(s, carry):
        j = s - BOTH
        q = s - LAG
        z = q - 1
        par = lax.rem(s, 2)
        arrives = (q >= 0) & (q < last)
        from_partner = (z >= 0) & (z < last)
        own_partner = (z >= 0) & (z < BOTH)
        pl.when(s == 2)(state_tail)
        pl.when((s >= 1) & (s <= BOTH))(lambda: stored(5))
        pl.when(s < BOTH)(lambda: own(s))

        @pl.when((j >= 0) & (j < HALF - LATE))
        def _():
            forward(1, xn, j, j).start()
            forward(0, yn, HALF + j, j).start()

        @pl.when((q >= 1) & (q <= last))
        def _():
            for a in pair:
                stored(a)

        @pl.when((z >= 1) & (z <= last))
        def _():
            for a in pair:
                stored(2 + a)

        pl.when((z >= 1) & (z <= BOTH))(lambda: stored(4))

        @pl.when(arrives)
        def _():
            for a in pair:
                seg, chunk = link_piece(q, a)
                link_wait(a, q).wait_recv()
                pl.when(q >= 2)(hand(a, par, q, at(0, 0), at(0, 0)).wait_send)

                def act(ref, a=a, seg=seg, chunk=chunk):
                    hand(a, par, q, ref, at(seg, chunk)).start()
                    fetch(a, ref)
                place(a, seg, chunk, q, act)

        @pl.when(own_partner)
        def _():
            remote(at(0, 0), at(0, 0), su.at[2, 0], ru_o.at[z], partner).wait_recv()
            fetch(4, at(partner, z))

        @pl.when(from_partner)
        def _():
            for a in pair:
                seg, chunk = link_piece(z, a)
                hand(a, 0, z, at(0, 0), at(0, 0)).wait_recv()
                fetch(2 + a, at(seg + flip, chunk))

        @pl.when(arrives)
        def _():
            for a in pair:
                convert(a, *link_piece(q, a))

        pl.when(own_partner)(lambda: convert(4, partner, z))

        @pl.when(from_partner)
        def _():
            for a in pair:
                seg, chunk = link_piece(z, a)
                convert(2 + a, seg + flip, chunk)
        return carry

    lax.fori_loop(0, last + LAG + 1, gather_step, 0)
    gains_finish()
    for a in pair:
        stored(2 + a)
        for par in pair:
            hand(a, par, 0, at(0, 0), at(0, 0)).wait_send()
        for j in range(HALF - LATE):
            forward(a, 0, 0, j).wait_send()
    for a in trio:
        local(st.at[a], outs[a].at[pl.ds(0, ROWS)], l_out.at[a]).wait()
        for ring in range(RING):
            remote(stage_u.at[ring], at(me, 0), su.at[a, ring], ru_o.at[0], partner).wait_send()


def copy_kernel(*args):
    ins, outs, (wide, thin, l_in, l_out) = args[:10], args[10:20], args[20:]
    depth = wide.shape[0]
    jobs = []
    for src, dst in zip(ins, outs):
        size, kind = src.shape[0], len(src.shape) - 2
        piece = (SEG_ROWS // 8, COUNTS[1])[kind]
        for off in range(0, size, piece):
            rows = pl.ds(off, min(piece, size - off))
            n = len(jobs)
            buf = (wide, thin)[kind].at[n % depth, pl.ds(0, rows.size)]
            jobs.append((local(src.at[rows], buf, l_in.at[n % depth]), local(buf, dst.at[rows], l_out.at[n % depth])))
    ahead = depth // 2
    for n in range(len(jobs) + ahead):
        if n < len(jobs):
            if n >= depth:
                jobs[n - depth][1].wait()
            jobs[n][0].start()
        if n >= ahead:
            jobs[n - ahead][0].wait()
            jobs[n - ahead][1].start()
    for job in jobs[-depth:]:
        job[1].wait()


def late_kernel(mine, *args):
    came, outs7 = args[:2], args[9:16]
    cin, cout, l_in, l_out = args[16:]
    flip, partner, xn, yn, diag = neighbours(lax.axis_index("dp"))
    seg = diag if mine else diag + flip
    jobs = [(a, i, a * LATE + i) for a in range(2) for i in range(LATE)]
    loads = [local(came[a].at[pl.ds(i * N, N)], cin.at[k], l_in.at[k]) for a, i, k in jobs]
    for load in loads:
        load.start()
    for a, i, k in jobs:
        loads[k].wait()

        def conv(d, k=k):
            cout[k, d] = cin[k, d].astype(BF16)
        tiles_loop(conv)
        store_piece(outs7, seg, ((1 + a) * HALF - LATE + i) * N + 0 * seg, cout.at[k], l_out.at[k])
    for k in range(2 * LATE):
        local(cout.at[k], outs7[0].at[pl.ds(0, N)], l_out.at[k]).wait()


ANY = pl.BlockSpec(memory_space=pl.ANY)
VMEM = pl.BlockSpec(memory_space=pltpu.VMEM)
SMEM = pl.BlockSpec(memory_space=pltpu.SMEM)


def to_tiles(x):
    cols = x.shape[-1]
    lead = x.size // cols
    return x.reshape(lead // 8, 8, cols // LANES, LANES).transpose(0, 2, 1, 3).reshape(-1, 8, LANES)


def from_tiles(t, shape):
    cols = shape[-1]
    lead = t.size // cols
    return t.reshape(lead // 8, cols // LANES, 8, LANES).transpose(0, 2, 1, 3).reshape(shape)


def shapes(kind, dtype, *dims):
    return [kind(d, dtype) for d in dims]


def dmas(*dims):
    return [pltpu.SemaphoreType.DMA(d) if d else pltpu.SemaphoreType.DMA for d in dims]


def params_of(**kw):
    return pltpu.CompilerParams(vmem_limit_bytes=LIMIT, has_side_effects=True, **kw)


def copy_call(arrays):
    depth = 12
    moved = 2 * sum(a.size * a.dtype.itemsize for a in arrays)
    return pl.pallas_call(
        copy_kernel,
        out_shape=[jax.ShapeDtypeStruct(a.shape, a.dtype) for a in arrays],
        in_specs=[ANY] * 10,
        out_specs=[ANY] * 10,
        scratch_shapes=[pltpu.VMEM((depth, SEG_ROWS // 8, LANES), F32), pltpu.VMEM((depth, COUNTS[1], 8, LANES), BF16)] + dmas((depth,), (depth,)),
        compiler_params=params_of(),
        cost_estimate=pl.CostEstimate(flops=100 * moved, bytes_accessed=moved, transcendentals=0),
        name="copy_results",
    )(*arrays)


def late_call(mine, came, tiles):
    chunks = 2 * LATE
    return pl.pallas_call(
        functools.partial(late_kernel, mine),
        out_shape=[jax.ShapeDtypeStruct(a.shape, a.dtype) for a in tiles],
        in_specs=[ANY] * 9,
        out_specs=[ANY] * 7,
        input_output_aliases={2 + k: k for k in range(7)},
        scratch_shapes=[pltpu.VMEM((chunks, N, 8, LANES), F32), pltpu.VMEM((chunks, N, 8, LANES), BF16)] + dmas((chunks,), (chunks,)),
        compiler_params=params_of(),
        cost_estimate=pl.CostEstimate(flops=came[0].size * 1000, bytes_accessed=came[0].size * 12, transcendentals=0),
        name="late_chunks",
    )(*came, *tiles)


def local_step(*arrays):
    grads = arrays[:10]
    states = [a.reshape(LOCAL_ROWS, LANES) for a in arrays[10:13]]
    chunk = (N, 8, LANES)
    sds = jax.ShapeDtypeStruct
    vm = pltpu.VMEM
    deep = len(FRONT)
    late = (LATE * N, 8, LANES)
    two, three, eight, width = 2, 3, 8, 1152
    tile, tail, long = (eight, LANES), (56, LANES), (104, LANES)
    res = pl.pallas_call(
        step_kernel,
        out_shape=shapes(sds, F32, *[(LOCAL_ROWS, LANES)] * three) + shapes(sds, BF16, *[(c, eight, LANES) for c in COUNTS], (two, width), (two, width), (1, width))
        + shapes(sds, F32, (eight, LANES), (SEG_ROWS + TAIL, LANES), (two, SLOTS) + chunk, (2 * SLOTS + BOTH,) + chunk, (eight, SEG_TILES, eight, LANES), late, late),
        in_specs=[ANY] * 7 + [VMEM] * 3 + [ANY] * 3 + [SMEM],
        out_specs=[ANY] * 10 + [VMEM] * 4 + [ANY] * 6,
        scratch_shapes=shapes(vm, BF16, (three, two) + chunk)
        + shapes(vm, F32, (three, two) + chunk, (RING,) + chunk, (two, two) + chunk, (RING, two) + chunk, (two, three) + chunk, (two, ROWS, LANES),
                 tile, (eight, *tile), tile)
        + shapes(vm, BF16, (deep, 24, eight, LANES))
        + shapes(vm, F32, (eight, 192, LANES), (deep, TAIL, LANES), (TAIL, LANES), (three, *tail), (three, *long), long, tail, tail,
                 (ROWS + TAIL, LANES), (three, ROWS, LANES), (ROWS + TAIL, LANES), (5,) + chunk)
        + shapes(vm, BF16, (6,) + chunk)
        + dmas((RING, two), (three, two), (two, SLOTS), (2 * SLOTS + BOTH,), (three, two), (two, two), (two, three), (two,), (deep,), (eight,),
               (deep,), (deep,), (deep,), (6,), None, None, None, (three,), (deep,), None,
               (three, RING), (two, SLOTS), (BOTH,), (two, SLOTS), (two, HALF), (two, two), (4,), (three,), (5,), (6,)),
        compiler_params=params_of(collective_id=0),
        name="adamw_step",
    )(*[to_tiles(x) for x in grads[:7]], *grads[7:], *states, arrays[13].reshape(1))
    kept, (norm, spare_x, spare_y) = res[:10], (res[13], res[18], res[19])

    def swap(x, bit):
        return lax.ppermute(x, "dp", [(i, i ^ bit) for i in range(8)])
    came = (swap(spare_x, 4), swap(spare_y, 2))
    copied = list(copy_call(kept))
    *came, copied[4] = lax.optimization_barrier((*came, copied[4]))
    tiles = late_call(True, came, copied[3:])
    tiles = late_call(False, [swap(c, 1) for c in came], tiles)
    params = [from_tiles(t, x.shape[1:]) for t, x in zip(tiles, grads[:7])]
    return tuple([a.reshape(-1) for a in copied[:3]] + params + [res[10], res[11], res[12].reshape(-1), norm[0, 0]])


def solution(mesh):
    return jax.shard_map(local_step, mesh=mesh, in_specs=(P("dp"),) * 13 + (P(),), out_specs=(P("dp"),) * 3 + (P(),) * 11, check_vma=False)
```

```python
import functools
import jax
import jax.numpy as jnp
from jax import lax
from jax.experimental import pallas as pl
from jax.experimental.pallas import tpu as pltpu
from jax.sharding import PartitionSpec as P

BETA_ONE = 0.9
BETA_TWO = 0.95
ADAM_EPS = 1e-8
WEIGHT_DECAY = 0.1
MAX_NORM = 1.0
CLIP_EPS = 1e-6
STEP = 4
BIAS_ONE = 1.0 - BETA_ONE ** STEP
BIAS_TWO = 1.0 - BETA_TWO ** STEP

MESH = pl.DeviceIdType.MESH
F32 = jnp.float32
BF16 = jnp.bfloat16
LANES = 128
SEG_TILES = 3456
SEG_ROWS = SEG_TILES * 8
LOCAL_ROWS = SEG_ROWS + 6
MATRIX_ROWS = 8 * SEG_ROWS
TAIL = 48
WIN = 27600
N = 144
ROWS = N * 8
HALF = SEG_TILES // 2 // N
BOTH = 2 * HALF
SLOTS = 3 * HALF
LATE = 5
RING = 4
LAG = 5
COUNTS = (2592, 864, 864, 2592, 6912, 6912, 6912)
FRONT = ((2, 0, 6, 3),) + tuple((k, t, 24, 24) for k in (4, 5) for t in (0, SEG_TILES)) + tuple((6, t, 9, 9) for t in (0, SEG_TILES))
LIMIT = 62 * 1024 * 1024


def neighbours(me):
    core = lax.rem(me, 2)
    x = lax.rem(lax.div(me, 2), 2)
    y = lax.div(me, 4)
    flip = 1 - 2 * core
    xn = me + 2 - 4 * x
    yn = me + 4 - 8 * y
    diag = xn + 4 - 8 * y
    return flip, me + flip, xn, yn, diag


def on_piece(refs, seg, tile, act):
    wq, wk, wv, wo, gate, up, down = refs
    pl.when((seg == 0) & (tile < 2592))(lambda: act(wq, tile))
    pl.when((seg == 0) & (tile >= 2592))(lambda: act(wk, tile - 2592))
    pl.when((seg == 1) & (tile < 864))(lambda: act(wv, tile))
    pl.when((seg == 1) & (tile >= 864))(lambda: act(wo, tile - 864))
    pl.when((seg == 2) | (seg == 3))(lambda: act(gate, (seg - 2) * SEG_TILES + tile))
    pl.when((seg == 4) | (seg == 5))(lambda: act(up, (seg - 4) * SEG_TILES + tile))
    pl.when((seg == 6) | (seg == 7))(lambda: act(down, (seg - 6) * SEG_TILES + tile))


def on_width(seg, tile, act):
    narrow = ((seg == 0) & (tile >= 2592)) | ((seg == 1) & (tile < 864))
    wide = (seg >= 2) & (seg < 6)
    pl.when(wide)(lambda: act(24))
    pl.when(narrow)(lambda: act(3))
    pl.when(jnp.logical_not(wide | narrow))(lambda: act(9))


def load_piece(refs, seg, tile, buf, sem):
    def act(ref, off):
        pltpu.make_async_copy(ref.at[pl.ds(off, N)], buf, sem).start()
    on_piece(refs, seg, tile, act)


def store_piece(refs, seg, tile, buf, sem):
    def act(ref, off):
        pltpu.make_async_copy(buf, ref.at[pl.ds(off, N)], sem).start()
    on_piece(refs, seg, tile, act)


def tiles_loop(body, group=12):
    def step(i, carry):
        body(pl.ds(pl.multiple_of(i * group, group), group))
        return carry
    lax.fori_loop(0, N // group, step, 0)


def remote(src, dst, send, recv, dev):
    return pltpu.make_async_remote_copy(src_ref=src, dst_ref=dst, send_sem=send, recv_sem=recv, device_id=(dev,), device_id_type=MESH)


def greet(devs):
    barrier = pltpu.get_barrier_semaphore()
    for dev in devs:
        pl.semaphore_signal(barrier, inc=1, device_id=(dev,), device_id_type=MESH)
    pl.semaphore_wait(barrier, len(devs))


def adam(g, p, m, v, lr, decay):
    m = BETA_ONE * m + (1.0 - BETA_ONE) * g
    v = BETA_TWO * v + (1.0 - BETA_TWO) * g * g
    direction = (m * (1.0 / BIAS_ONE)) / (jnp.sqrt(v * (1.0 / BIAS_TWO)) + ADAM_EPS)
    return p - lr * (decay * p + direction), m, v


def local(src, dst, sem):
    return pltpu.make_async_copy(src, dst, sem)


def step_kernel(*args):
    refs, small, ins, rate = args[:7], args[7:10], args[10:13], args[13]
    outs, outs7, gains_out, o_norm = args[14:17], args[17:24], args[24:27], args[27]
    g_flat, land_l, land_p, land, spare_x, spare_y, end_x, end_y = args[28:36]
    (raw, stage_p, stage_u, aux, stage, own_in, own_g, norm_send, norm_land, n_out, front_raw, front, front_land, tail_g,
     window, halo, window_g, gains_send, gains_land, gb, st, pb, cin, cout) = args[36:60]
    (s_l, s_p, r_l, r_p, l_raw, l_aux, l_own, l_g, s_n, r_n, l_front, s_front, r_front, l_win, s_win, r_win, l_tail, l_six, s_gain, r_gain,
     su, ru, ru_o, r_d, s_f, s_d, l_in, l_out, l_c, l_so) = args[60:]
    spare, ends = (spare_x, spare_y), (end_x, end_y)
    me = lax.axis_index("dp")
    flip, partner, xn, yn, diag = neighbours(me)
    links = (xn, yn)
    pair = range(len(links))
    trio = range(len(ins))
    others = [lax.rem(me + o, 8) for o in range(1, 8)]
    shift = 6 * me
    lr = rate[0]
    n_out[...] = jnp.zeros_like(n_out)
    window[...] = jnp.zeros_like(window)
    window_g[...] = jnp.zeros_like(window_g)
    halo[:, pl.ds(56, TAIL), :] = jnp.zeros((3, TAIL, LANES), F32)
    front[7] = jnp.zeros(front.shape[1:], F32)

    def raw_wait(kind, a):
        local(refs[0].at[pl.ds(0, N)], raw.at[kind, a], l_raw.at[kind, a]).wait()

    def to_partner(par, a, slot):
        return remote(stage_p.at[par, a], land_p.at[slot], s_p.at[par, a], r_p.at[slot], partner)

    def to_link(ring, a, slot):
        return remote(stage.at[ring, a], land_l.at[a, slot], s_l.at[ring, a], r_l.at[a, slot], links[a])

    def window_copies():
        out = []
        for a in trio:
            for row, place, rows in ((WIN, 0, TAIL), (SEG_ROWS, TAIL, 6)):
                out.append(local(ins[a].at[pl.ds(row, rows)], window.at[a, pl.ds(place, rows)], l_win.at[len(out)]))
        return out

    def front_copies():
        return [local(refs[k].at[pl.ds(off, cnt)], front_raw.at[d, pl.ds(0, cnt)], l_front.at[d]) for d, (k, off, cnt, width) in enumerate(FRONT)]

    def front_sends():
        return [remote(front.at[dev, pl.ds(0, TAIL)], front_land.at[o], s_front.at[o], r_front.at[o], dev) for o, dev in enumerate(others)]

    def window_send():
        return remote(window, halo.at[:, pl.ds(0, 56)], s_win, r_win, others[0])

    def small_exchange():
        for copy in window_copies() + front_copies():
            copy.start()
        place = 0
        for ref, count in zip(small, (2, 2, 1)):
            value = ref[...].reshape(count, 9 * LANES).astype(F32)
            for r in range(count):
                for w in range(9):
                    front[7, pl.ds(place, 1), :] = value[r:r + 1, w * LANES:(w + 1) * LANES]
                    place += 1
        for copy in window_copies() + front_copies():
            copy.wait()
        for d, (k, off, cnt, width) in enumerate(FRONT):
            for t in range(cnt):
                front[d, pl.ds(t // width * 8 * width + t % width, 8, stride=width), :] = front_raw[d, t].astype(F32)
        window_send().start()
        for copy in front_sends():
            copy.start()

    def small_finish():
        total = front[me, pl.ds(0, TAIL), :]
        for o, copy in enumerate(front_sends()):
            copy.wait()
            total = total + front_land[o]
        window_send().wait()
        total = total * 0.125
        tail_g[...] = total

        @pl.when(me == 7)
        def _():
            n_out[...] += jnp.sum((total * total).reshape(TAIL // 8, 8, LANES), axis=0)
        copy = local(tail_g, g_flat.at[pl.ds(SEG_ROWS, TAIL)], l_tail)
        copy.start()
        copy.wait()

    def link_jobs(s):
        jobs = []
        for a in pair:
            half = jnp.where(s < BOTH, a, 1 - a)
            seg = jnp.where(s < HALF, diag, links[a])
            jobs.append((seg, (half * HALF + lax.rem(s, HALF)) * N, a * SLOTS + s))
        return jobs

    def own_jobs(j):
        return [(me, (h * HALF + j) * N, 2 * SLOTS + h * HALF + j) for h in pair]

    def raw_loads(jobs, kind, turn):
        for a, (seg, tile, slot) in enumerate(jobs):
            load_piece(refs, seg + turn, tile, raw.at[kind, a], l_raw.at[kind, a])

    def give(jobs, kind, par, wait_old, load=True):
        if load:
            raw_loads(jobs, kind, flip)
        for a, (seg, tile, slot) in enumerate(jobs):
            raw_wait(kind, a)
            copy = to_partner(par, a, slot)
            pl.when(wait_old)(copy.wait_send)

            def conv(d, a=a):
                stage_p[par, a, d] = raw[kind, a, d].astype(F32)
            tiles_loop(conv)
            copy.start()

    def step(s, count):
        j = lax.rem(s, HALF)
        ring = lax.rem(s, RING)

        @pl.when(s < SLOTS - 1)
        def _():
            give(link_jobs(s + 1), 0, lax.rem(s + 1, 2), s >= 1)

        @pl.when(s < SLOTS)
        def _():
            jobs = link_jobs(s)
            pl.when(s >= 1)(lambda: raw_loads(jobs, 1, 0))
            for a, (seg, tile, slot) in enumerate(jobs):
                to_partner(0, a, slot).wait_recv()
                local(land_p.at[slot], aux.at[0, a], l_aux.at[0, a]).start()

            @pl.when(s >= BOTH)
            def _():
                for a in pair:
                    to_link(0, a, j).wait_recv()
                for a in pair:
                    local(land_l.at[1 - a, j], aux.at[1, a], l_aux.at[1, a]).start()
            for a in pair:
                raw_wait(1, a)
                local(land_p.at[0], aux.at[0, a], l_aux.at[0, a]).wait()
                copy = to_link(ring, a, s)
                pl.when(s >= RING)(copy.wait_send)

                @pl.when(s < BOTH)
                def _(a=a):
                    def add(d):
                        stage[ring, a, d] = raw[1, a, d].astype(F32) + aux[0, a, d]
                    tiles_loop(add)

                @pl.when(s >= BOTH)
                def _(a=a):
                    local(land_p.at[0], aux.at[1, a], l_aux.at[1, a]).wait()

                    def add(d):
                        stage[ring, a, d] = raw[1, a, d].astype(F32) + aux[0, a, d] + aux[1, a, d]
                    tiles_loop(add)
                copy.start()

        pl.when(s == 2)(small_exchange)
        pl.when(s == BOTH + 4)(small_finish)

        @pl.when((s >= HALF + 4) & (s < BOTH + 4))
        def _():
            give(own_jobs(s - HALF - 4), 2, 2, s > HALF + 4)

        @pl.when(s >= BOTH + LAG)
        def _():
            take_own(s - BOTH - LAG)
        return count

    def take_own(j):
        for h, (seg, tile, slot) in enumerate(own_jobs(j)):
            load_piece(refs, seg, tile, raw.at[2, h], l_raw.at[2, h])
            to_partner(2, h, slot).wait_recv()
            local(land_p.at[slot], own_in.at[h, 0], l_own.at[h, 0]).start()
        for k in (1, 2):
            for h in pair:
                a = h if k == 1 else 1 - h
                slot = k * HALF + j
                to_link(0, a, slot).wait_recv()
                local(land_l.at[a, slot], own_in.at[h, k], l_own.at[h, k]).start()
        for h, (seg, tile, slot) in enumerate(own_jobs(j)):
            raw_wait(2, h)
            for a in trio:
                local(land_p.at[0], own_in.at[h, a], l_own.at[h, a]).wait()
            row = pl.multiple_of(tile * 8, 8)
            out = local(own_g.at[h], g_flat.at[pl.ds(row, ROWS)], l_g.at[h])
            pl.when(j >= 1)(out.wait)

            def relay(width, h=h):
                def body(r, acc):
                    for w in range(width):
                        t = r * width + w
                        g = (raw[2, h, t].astype(F32) + own_in[h, 0, t] + own_in[h, 1, t] + own_in[h, 2, t]) * 0.125
                        own_g[h, pl.ds(r * (8 * width) + w, 8, stride=width), :] = g
                        acc = acc + g * g
                    return acc
                n_out[...] += lax.fori_loop(0, N // width, body, jnp.zeros((8, LANES), F32))
            on_width(me, tile, relay)
            out.start()

    def state_loads(s):
        row, par = pl.multiple_of(s * ROWS, 8), lax.rem(s, 2)
        return [local(ins[a].at[pl.ds(row, ROWS)], st.at[par, a], l_in.at[par, a]) for a in trio]

    def gradient_load(s):
        row, par = pl.multiple_of(s * ROWS, 8), lax.rem(s, 2)
        return local(g_flat.at[pl.ds(row, ROWS + TAIL)], gb.at[par], l_in.at[par, 3])

    raw_loads(link_jobs(0), 0, flip)
    raw_loads(link_jobs(0), 1, 0)
    greet(others)
    give(link_jobs(0), 0, 0, False, False)
    lax.fori_loop(0, SLOTS + LAG, step, 0)
    for load in state_loads(0):
        load.start()
    gradient_load(0).start()

    norm_send[...] = n_out[...]
    norm_land[me] = n_out[...]

    def norm_copy(o, dev, slot):
        return remote(norm_send, norm_land.at[slot], s_n.at[o], r_n.at[slot], dev)
    for o, dev in enumerate(others):
        norm_copy(o, dev, me).start()
    for h in pair:
        local(own_g.at[h], g_flat.at[pl.ds(0, ROWS)], l_g.at[h]).wait()
    for o, dev in enumerate(others):
        norm_copy(o, dev, me).wait_send()
        norm_copy(o, dev, dev).wait_recv()
    n_out[...] = jnp.sum(norm_land[...], axis=0)
    norm = jnp.sqrt(jnp.sum(n_out[...], axis=(0, 1), keepdims=True))
    o_norm[...] = jnp.broadcast_to(norm, (8, LANES))
    n_out[...] = jnp.broadcast_to(jnp.minimum(1.0, MAX_NORM / (norm + CLIP_EPS)), (8, LANES))
    coef = n_out[pl.ds(0, 1), :]
    for a in pair:
        for par in trio:
            to_partner(par, a, 0).wait_send()
        for ring in range(RING):
            to_link(ring, a, 0).wait_send()

    def state_tail():
        copy = local(g_flat.at[pl.ds(WIN, 2 * TAIL)], window_g.at[pl.ds(0, 2 * TAIL)], l_tail)
        copy.start()
        copy.wait()
        place = lax.broadcasted_iota(jnp.int32, (56, LANES), 0) + (me * LOCAL_ROWS + WIN)
        decay = jnp.where(place < MATRIX_ROWS, WEIGHT_DECAY, 0.0)
        new = adam(window_g[pl.ds(shift, 56), :] * coef, window[0], window[1], window[2], lr, decay)
        gains_send[...] = new[0]
        for a in trio:
            window[a] = new[a]
            six_store(a).start()

        @pl.when(me == 7)
        def _():
            for o, dev in enumerate(others):
                gains_copy(o, dev).start()

    def six_store(a):
        return local(window.at[a, pl.ds(TAIL, 6)], outs[a].at[pl.ds(SEG_ROWS, 6)], l_six.at[a])

    def gains_copy(o, dev):
        return remote(gains_send, gains_land, s_gain.at[o], r_gain, dev)

    def gains_finish():
        def write(src):
            t = src[...]

            def row(r):
                return jnp.concatenate([t[6 + 9 * r + w:7 + 9 * r + w, :] for w in range(9)], axis=1)
            for out, rows in zip(gains_out, ((0, 1), (2, 3), (4,))):
                out[...] = jnp.concatenate([row(r) for r in rows], axis=0).astype(BF16)

        @pl.when(me == 7)
        def _():
            for o, dev in enumerate(others):
                gains_copy(o, dev).wait_send()
            write(gains_send)

        @pl.when(me != 7)
        def _():
            gains_copy(0, others[0]).wait_recv()
            write(gains_land)
        for a in trio:
            six_store(a).wait()

    def first_rows():
        part = pl.ds(54 - shift, TAIL)
        pb[pl.ds(0, TAIL), :] = adam(gb[0, pl.ds(0, TAIL), :] * coef, *[halo[a, part, :] for a in trio], lr, WEIGHT_DECAY)[0]

    def at(seg, c):
        return land.at[seg, pl.ds(pl.multiple_of(c * N, N), N)]

    def place(a, seg, chunk, q, act):
        low = (1 + a) * HALF - LATE
        late = (q >= low) & (q < low + LATE)
        pl.when(late)(lambda: act(spare[a].at[pl.ds((q - low) * N, N)]))
        pl.when(jnp.logical_not(late))(lambda: act(at(seg, chunk)))

    def link_piece(q, a):
        direct = q < BOTH
        return jnp.where(direct, links[a], diag), jnp.where(direct, q, q - (1 + a) * HALF)

    def own(s):
        ring = lax.rem(s, RING)
        row = pl.multiple_of(s * ROWS, 8)

        par = lax.rem(s, 2)

        def state_store(a, par):
            return local(st.at[par, a], outs[a].at[pl.ds(row, ROWS)], l_out.at[par, a])

        @pl.when(s < BOTH - 1)
        def _():
            gradient_load(s + 1).start()
            for a, load in enumerate(state_loads(s + 1)):
                pl.when(s >= 1)(state_store(a, 1 - par).wait)
                load.start()
        for load in state_loads(s) + [gradient_load(s)]:
            load.wait()
        pl.when(s == 0)(first_rows)
        slab = 48
        base = me * LOCAL_ROWS + s * ROWS

        def update(i, carry):
            d = pl.ds(pl.multiple_of(i * slab, 8), slab)
            e = pl.ds(i * slab + shift, slab)
            rows = lax.broadcasted_iota(jnp.int32, (slab, LANES), 0) + (base + i * slab)
            decay = jnp.where(rows < MATRIX_ROWS, WEIGHT_DECAY, 0.0)
            new = adam(gb[par, e, :] * coef, *[st[par, a, d, :] for a in trio], lr, decay)
            for a in trio:
                st[par, a, d, :] = new[a]
            pb[e, :] = new[0]
            return carry
        lax.fori_loop(0, ROWS // slab, update, 0)
        for a in trio:
            state_store(a, par).start()
        devs = links + (partner,)

        @pl.when(s >= RING)
        def _():
            for a in trio:
                remote(stage_u.at[ring], at(me, s), su.at[a, ring], ru_o.at[s], devs[a]).wait_send()

        def relay(width):
            def body(r, carry):
                for w in range(width):
                    stage_u[ring, r * width + w] = pb[pl.ds(r * (8 * width) + w, 8, stride=width), :]
                return carry
            lax.fori_loop(0, N // width, body, 0)
        on_width(me, s * N, relay)
        pb[pl.ds(0, TAIL), :] = pb[pl.ds(ROWS, TAIL), :]
        for a in pair:
            place(a, me, s, s, lambda ref, a=a: remote(stage_u.at[ring], ref, su.at[a, ring], ru.at[a, s], devs[a]).start())
        remote(stage_u.at[ring], at(me, s), su.at[2, ring], ru_o.at[s], partner).start()

        def conv(d):
            cout[5, d] = stage_u[ring, d].astype(BF16)
        tiles_loop(conv)
        store_piece(outs7, me, s * N, cout.at[5], l_so.at[5])

    def convert(k, seg, chunk):
        local(at(0, 0), cin.at[k], l_c.at[k]).wait()

        def conv(d):
            cout[k, d] = cin[k, d].astype(BF16)
        tiles_loop(conv)
        store_piece(outs7, seg, chunk * N, cout.at[k], l_so.at[k])

    def fetch(k, ref):
        local(ref, cin.at[k], l_c.at[k]).start()

    def stored(k):
        local(cout.at[k], outs7[0].at[pl.ds(0, N)], l_so.at[k]).wait()

    last = SLOTS - LATE - 1
    spot = at(0, 0)

    def link_wait(a, q):
        return remote(spot, spot, s_d.at[a, 0], ru.at[a, q], links[a])

    def hand(a, par, q, src, dst):
        return remote(src, dst, s_d.at[a, par], r_d.at[a, q], partner)

    def forward(a, seg, chunk, j, dst):
        return remote(at(seg, chunk), dst, s_f.at[a, j], ru.at[a, BOTH + j], links[a])

    def start_forward(a, seg, chunk, j):
        pl.when(j < HALF - LATE - 1)(lambda: forward(a, seg, chunk, j, at(seg, chunk)).start())
        pl.when(j == HALF - LATE - 1)(lambda: forward(a, seg, chunk, j, ends[a]).start())

    def gather_step(s, carry):
        j = s - BOTH
        q = s - LAG
        z = q - 1
        par = lax.rem(s, 2)
        arrives = (q >= 0) & (q < last)
        from_partner = (z >= 0) & (z < last)
        own_partner = (z >= 0) & (z < BOTH)
        pl.when(s == 2)(state_tail)
        pl.when((s >= 1) & (s <= BOTH))(lambda: stored(5))
        pl.when(s < BOTH)(lambda: own(s))

        @pl.when((j >= 0) & (j < HALF - LATE))
        def _():
            start_forward(1, xn, j, j)
            start_forward(0, yn, HALF + j, j)

        @pl.when((q >= 1) & (q <= last))
        def _():
            for a in pair:
                stored(a)

        @pl.when((z >= 1) & (z <= last))
        def _():
            for a in pair:
                stored(2 + a)

        pl.when((z >= 1) & (z <= BOTH))(lambda: stored(4))

        @pl.when(arrives)
        def _():
            for a in pair:
                seg, chunk = link_piece(q, a)
                link_wait(a, q).wait_recv()
                pl.when(q >= 2)(hand(a, par, q, spot, spot).wait_send)

                def act(ref, a=a, seg=seg, chunk=chunk):
                    hand(a, par, q, ref, at(seg, chunk)).start()
                    fetch(a, ref)
                place(a, seg, chunk, q, act)

        @pl.when(own_partner)
        def _():
            remote(spot, spot, su.at[2, 0], ru_o.at[z], partner).wait_recv()
            fetch(4, at(partner, z))

        @pl.when(from_partner)
        def _():
            for a in pair:
                seg, chunk = link_piece(z, a)
                hand(a, 0, z, spot, spot).wait_recv()
                fetch(2 + a, at(seg + flip, chunk))

        @pl.when(arrives)
        def _():
            for a in pair:
                convert(a, *link_piece(q, a))

        pl.when(own_partner)(lambda: convert(4, partner, z))

        @pl.when(from_partner)
        def _():
            for a in pair:
                seg, chunk = link_piece(z, a)
                convert(2 + a, seg + flip, chunk)
        return carry

    lax.fori_loop(0, last + LAG + 1, gather_step, 0)
    gains_finish()
    for a in pair:
        link_wait(a, last).wait_recv()
    for a in pair:
        stored(2 + a)
        for par in pair:
            hand(a, par, 0, spot, spot).wait_send()
        for j in range(HALF - LATE):
            forward(a, 0, 0, j, spot).wait_send()
    for a in trio:
        for par in pair:
            local(st.at[par, a], outs[a].at[pl.ds(0, ROWS)], l_out.at[par, a]).wait()
        for ring in range(RING):
            remote(stage_u.at[ring], at(me, 0), su.at[a, ring], ru_o.at[0], partner).wait_send()


def copy_kernel(*args):
    ins, outs, (wide, thin, l_in, l_out) = args[:10], args[10:20], args[20:]
    depth = wide.shape[0]
    jobs = []
    for src, dst in zip(ins, outs):
        size, kind = src.shape[0], len(src.shape) - 2
        piece = (SEG_ROWS // 8, COUNTS[1])[kind]
        for off in range(0, size, piece):
            rows = pl.ds(off, min(piece, size - off))
            n = len(jobs)
            buf = (wide, thin)[kind].at[n % depth, pl.ds(0, rows.size)]
            jobs.append((local(src.at[rows], buf, l_in.at[n % depth]), local(buf, dst.at[rows], l_out.at[n % depth])))
    ahead = depth // 2
    for n in range(len(jobs) + ahead):
        if n < len(jobs):
            if n >= depth:
                jobs[n - depth][1].wait()
            jobs[n][0].start()
        if n >= ahead:
            jobs[n - ahead][0].wait()
            jobs[n - ahead][1].start()
    for job in jobs[-depth:]:
        job[1].wait()


def late_kernel(mine, *args):
    came, ends, outs7 = args[:2], args[2:4], args[11:18]
    cin, cout, l_in, l_out = args[18:]
    flip, partner, xn, yn, diag = neighbours(lax.axis_index("dp"))
    seg = diag if mine else diag + flip
    jobs = [(a, i, a * (LATE + 1) + i) for a in range(2) for i in range(LATE + 1)]
    loads = [local(came[a].at[pl.ds(i * N, N)] if i < LATE else ends[a], cin.at[k], l_in.at[k]) for a, i, k in jobs]
    for load in loads:
        load.start()
    for a, i, k in jobs:
        loads[k].wait()

        def conv(d, k=k):
            cout[k, d] = cin[k, d].astype(BF16)
        tiles_loop(conv)
        chunk = (1 + a) * HALF - LATE + (i if i < LATE else -1)
        store_piece(outs7, seg, chunk * N + 0 * seg, cout.at[k], l_out.at[k])
    for a, i, k in jobs:
        local(cout.at[k], outs7[0].at[pl.ds(0, N)], l_out.at[k]).wait()


ANY = pl.BlockSpec(memory_space=pl.ANY)
VMEM = pl.BlockSpec(memory_space=pltpu.VMEM)
SMEM = pl.BlockSpec(memory_space=pltpu.SMEM)


def to_tiles(x):
    cols = x.shape[-1]
    lead = x.size // cols
    return x.reshape(lead // 8, 8, cols // LANES, LANES).transpose(0, 2, 1, 3).reshape(-1, 8, LANES)


def from_tiles(t, shape):
    cols = shape[-1]
    lead = t.size // cols
    return t.reshape(lead // 8, cols // LANES, 8, LANES).transpose(0, 2, 1, 3).reshape(shape)


def shapes(kind, dtype, *dims):
    return [kind(d, dtype) for d in dims]


def dmas(*dims):
    return [pltpu.SemaphoreType.DMA(d) if d else pltpu.SemaphoreType.DMA for d in dims]


def params_of(**kw):
    return pltpu.CompilerParams(vmem_limit_bytes=LIMIT, has_side_effects=True, **kw)


def copy_call(arrays):
    depth = 12
    moved = 2 * sum(a.size * a.dtype.itemsize for a in arrays)
    return pl.pallas_call(
        copy_kernel,
        out_shape=[jax.ShapeDtypeStruct(a.shape, a.dtype) for a in arrays],
        in_specs=[ANY] * 10,
        out_specs=[ANY] * 10,
        scratch_shapes=[pltpu.VMEM((depth, SEG_ROWS // 8, LANES), F32), pltpu.VMEM((depth, COUNTS[1], 8, LANES), BF16)] + dmas((depth,), (depth,)),
        compiler_params=params_of(),
        cost_estimate=pl.CostEstimate(flops=100 * moved, bytes_accessed=moved, transcendentals=0),
        name="copy_results",
    )(*arrays)


def late_call(mine, came, tiles):
    chunks = 2 * LATE + 2
    return pl.pallas_call(
        functools.partial(late_kernel, mine),
        out_shape=[jax.ShapeDtypeStruct(a.shape, a.dtype) for a in tiles],
        in_specs=[ANY] * 11,
        out_specs=[ANY] * 7,
        input_output_aliases={4 + k: k for k in range(7)},
        scratch_shapes=[pltpu.VMEM((chunks, N, 8, LANES), F32), pltpu.VMEM((chunks, N, 8, LANES), BF16)] + dmas((chunks,), (chunks,)),
        compiler_params=params_of(),
        cost_estimate=pl.CostEstimate(flops=came[0].size * 1000, bytes_accessed=came[0].size * 12, transcendentals=0),
        name="late_chunks",
    )(*came, *tiles)


def local_step(*arrays):
    grads = arrays[:10]
    states = [a.reshape(LOCAL_ROWS, LANES) for a in arrays[10:13]]
    chunk = (N, 8, LANES)
    sds = jax.ShapeDtypeStruct
    vm = pltpu.VMEM
    deep = len(FRONT)
    late = (LATE * N, 8, LANES)
    two, three, eight, width = 2, 3, 8, 1152
    tile, tail, long = (eight, LANES), (56, LANES), (104, LANES)
    res = pl.pallas_call(
        step_kernel,
        out_shape=shapes(sds, F32, *[(LOCAL_ROWS, LANES)] * three) + shapes(sds, BF16, *[(c, eight, LANES) for c in COUNTS], (two, width), (two, width), (1, width))
        + shapes(sds, F32, (eight, LANES), (SEG_ROWS + TAIL, LANES), (two, SLOTS) + chunk, (2 * SLOTS + BOTH,) + chunk, (eight, SEG_TILES, eight, LANES), late, late, chunk, chunk),
        in_specs=[ANY] * 7 + [VMEM] * 3 + [ANY] * 3 + [SMEM],
        out_specs=[ANY] * 10 + [VMEM] * 4 + [ANY] * 8,
        scratch_shapes=shapes(vm, BF16, (three, two) + chunk)
        + shapes(vm, F32, (three, two) + chunk, (RING,) + chunk, (two, two) + chunk, (RING, two) + chunk, (two, three) + chunk, (two, ROWS, LANES),
                 tile, (eight, *tile), tile)
        + shapes(vm, BF16, (deep, 24, eight, LANES))
        + shapes(vm, F32, (eight, 192, LANES), (deep, TAIL, LANES), (TAIL, LANES), (three, *tail), (three, *long), long, tail, tail,
                 (two, ROWS + TAIL, LANES), (two, three, ROWS, LANES), (ROWS + TAIL, LANES), (5,) + chunk)
        + shapes(vm, BF16, (6,) + chunk)
        + dmas((RING, two), (three, two), (two, SLOTS), (2 * SLOTS + BOTH,), (three, two), (two, two), (two, three), (two,), (deep,), (eight,),
               (deep,), (deep,), (deep,), (6,), None, None, None, (three,), (deep,), None,
               (three, RING), (two, SLOTS), (BOTH,), (two, SLOTS), (two, HALF), (two, two), (two, 4), (two, three), (5,), (6,)),
        compiler_params=params_of(collective_id=0),
        name="adamw_step",
    )(*[to_tiles(x) for x in grads[:7]], *grads[7:], *states, arrays[13].reshape(1))
    kept, (norm, spare_x, spare_y) = res[:10], (res[13], *res[18:20])

    def swap(x, bit):
        return lax.ppermute(x, "dp", [(i, i ^ bit) for i in range(8)])
    ends = res[:-3:-1]
    came = [swap(spare_x, 4), swap(spare_y, 2)] + [swap(e, 1) for e in ends]
    copied = list(copy_call(kept))
    *came, copied[4] = lax.optimization_barrier((*came, copied[4]))
    tiles = late_call(True, (*came[:2], *ends), copied[3:])
    tiles = late_call(False, (*[swap(c, 1) for c in came[:2]], *came[2:]), tiles)
    params = [from_tiles(t, x.shape[1:]) for t, x in zip(tiles, grads[:7])]
    return tuple([a.reshape(-1) for a in copied[:3]] + params + [res[10], res[11], res[12].reshape(-1), norm[0, 0]])


def solution(mesh):
    return jax.shard_map(local_step, mesh=mesh, in_specs=(P("dp"),) * 13 + (P(),), out_specs=(P("dp"),) * 3 + (P(),) * 11, check_vma=False)
```

```python
import functools
import jax
import jax.numpy as jnp
from jax import lax
from jax.experimental import pallas as pl
from jax.experimental.pallas import tpu as pltpu
from jax.sharding import PartitionSpec as P

BETA_ONE = 0.9
BETA_TWO = 0.95
ADAM_EPS = 1e-8
WEIGHT_DECAY = 0.1
MAX_NORM = 1.0
CLIP_EPS = 1e-6
STEP = 4
BIAS_ONE = 1.0 - BETA_ONE ** STEP
BIAS_TWO = 1.0 - BETA_TWO ** STEP

MESH = pl.DeviceIdType.MESH
F32 = jnp.float32
BF16 = jnp.bfloat16
LANES = 128
SEG_TILES = 3456
SEG_ROWS = SEG_TILES * 8
LOCAL_ROWS = SEG_ROWS + 6
MATRIX_ROWS = 8 * SEG_ROWS
TAIL = 48
WIN = 27600
N = 144
ROWS = N * 8
HALF = SEG_TILES // 2 // N
BOTH = 2 * HALF
SLOTS = 3 * HALF
LATE = 5
RING = 4
LAG = 5
COUNTS = (2592, 864, 864, 2592, 6912, 6912, 6912)
FRONT = ((2, 0, 6, 3),) + tuple((k, t, 24, 24) for k in (4, 5) for t in (0, SEG_TILES)) + tuple((6, t, 9, 9) for t in (0, SEG_TILES))
LIMIT = 62 * 1024 * 1024


def neighbours(me):
    core = lax.rem(me, 2)
    x = lax.rem(lax.div(me, 2), 2)
    y = lax.div(me, 4)
    flip = 1 - 2 * core
    xn = me + 2 - 4 * x
    yn = me + 4 - 8 * y
    diag = xn + 4 - 8 * y
    return flip, me + flip, xn, yn, diag


def on_piece(refs, seg, tile, act):
    wq, wk, wv, wo, gate, up, down = refs
    pl.when((seg == 0) & (tile < 2592))(lambda: act(wq, tile))
    pl.when((seg == 0) & (tile >= 2592))(lambda: act(wk, tile - 2592))
    pl.when((seg == 1) & (tile < 864))(lambda: act(wv, tile))
    pl.when((seg == 1) & (tile >= 864))(lambda: act(wo, tile - 864))
    pl.when((seg == 2) | (seg == 3))(lambda: act(gate, (seg - 2) * SEG_TILES + tile))
    pl.when((seg == 4) | (seg == 5))(lambda: act(up, (seg - 4) * SEG_TILES + tile))
    pl.when((seg == 6) | (seg == 7))(lambda: act(down, (seg - 6) * SEG_TILES + tile))


def on_width(seg, tile, act):
    narrow = ((seg == 0) & (tile >= 2592)) | ((seg == 1) & (tile < 864))
    wide = (seg >= 2) & (seg < 6)
    pl.when(wide)(lambda: act(24))
    pl.when(narrow)(lambda: act(3))
    pl.when(jnp.logical_not(wide | narrow))(lambda: act(9))


def load_piece(refs, seg, tile, buf, sem):
    def act(ref, off):
        pltpu.make_async_copy(ref.at[pl.ds(off, N)], buf, sem).start()
    on_piece(refs, seg, tile, act)


def store_piece(refs, seg, tile, buf, sem):
    def act(ref, off):
        pltpu.make_async_copy(buf, ref.at[pl.ds(off, N)], sem).start()
    on_piece(refs, seg, tile, act)


def tiles_loop(body, group=12):
    def step(i, carry):
        body(pl.ds(pl.multiple_of(i * group, group), group))
        return carry
    lax.fori_loop(0, N // group, step, 0)


def remote(src, dst, send, recv, dev):
    return pltpu.make_async_remote_copy(src_ref=src, dst_ref=dst, send_sem=send, recv_sem=recv, device_id=(dev,), device_id_type=MESH)


def greet(devs):
    barrier = pltpu.get_barrier_semaphore()
    for dev in devs:
        pl.semaphore_signal(barrier, inc=1, device_id=(dev,), device_id_type=MESH)
    pl.semaphore_wait(barrier, len(devs))


def adam(g, p, m, v, lr, decay):
    m = BETA_ONE * m + (1.0 - BETA_ONE) * g
    v = BETA_TWO * v + (1.0 - BETA_TWO) * g * g
    direction = (m * (1.0 / BIAS_ONE)) / (jnp.sqrt(v * (1.0 / BIAS_TWO)) + ADAM_EPS)
    return p - lr * (decay * p + direction), m, v


def local(src, dst, sem):
    return pltpu.make_async_copy(src, dst, sem)


def step_kernel(*args):
    refs, small, ins, rate = args[:7], args[7:10], args[10:13], args[13]
    outs, outs7, gains_out, o_norm = args[14:17], args[17:24], args[24:27], args[27]
    g_flat, land_l, land_p, land, spare_x, spare_y, end_x, end_y = args[28:36]
    (raw, stage_p, stage_u, aux, stage, own_in, own_g, norm_send, norm_land, n_out, front_raw, front, front_land, tail_g,
     window, halo, window_g, gains_send, gains_land, gb, st, pb, cin, cout) = args[36:60]
    (s_l, s_p, r_l, r_p, l_raw, l_aux, l_own, l_g, s_n, r_n, l_front, s_front, r_front, l_win, s_win, r_win, l_tail, l_six, s_gain, r_gain,
     su, ru, ru_o, r_d, s_f, s_d, l_in, l_out, l_c, l_so) = args[60:]
    spare, ends = (spare_x, spare_y), (end_x, end_y)
    me = lax.axis_index("dp")
    flip, partner, xn, yn, diag = neighbours(me)
    links = (xn, yn)
    pair = range(len(links))
    trio = range(len(ins))
    others = [lax.rem(me + o, 8) for o in range(1, 8)]
    shift = 6 * me
    lr = rate[0]
    n_out[...] = jnp.zeros_like(n_out)
    window[...] = jnp.zeros_like(window)
    window_g[...] = jnp.zeros_like(window_g)
    halo[:, pl.ds(56, TAIL), :] = jnp.zeros((3, TAIL, LANES), F32)
    front[7] = jnp.zeros(front.shape[1:], F32)

    def raw_wait(kind, a):
        local(refs[0].at[pl.ds(0, N)], raw.at[kind, a], l_raw.at[kind, a]).wait()

    def to_partner(par, a, slot):
        return remote(stage_p.at[par, a], land_p.at[slot], s_p.at[par, a], r_p.at[slot], partner)

    def to_link(ring, a, slot):
        return remote(stage.at[ring, a], land_l.at[a, slot], s_l.at[ring, a], r_l.at[a, slot], links[a])

    def window_copies():
        out = []
        for a in trio:
            for row, place, rows in ((WIN, 0, TAIL), (SEG_ROWS, TAIL, 6)):
                out.append(local(ins[a].at[pl.ds(row, rows)], window.at[a, pl.ds(place, rows)], l_win.at[len(out)]))
        return out

    def front_copies():
        return [local(refs[k].at[pl.ds(off, cnt)], front_raw.at[d, pl.ds(0, cnt)], l_front.at[d]) for d, (k, off, cnt, width) in enumerate(FRONT)]

    def front_sends():
        return [remote(front.at[dev, pl.ds(0, TAIL)], front_land.at[o], s_front.at[o], r_front.at[o], dev) for o, dev in enumerate(others)]

    def window_send():
        return remote(window, halo.at[:, pl.ds(0, 56)], s_win, r_win, others[0])

    def small_exchange():
        for copy in window_copies() + front_copies():
            copy.start()
        place = 0
        for ref, count in zip(small, (2, 2, 1)):
            value = ref[...].reshape(count, 9 * LANES).astype(F32)
            for r in range(count):
                for w in range(9):
                    front[7, pl.ds(place, 1), :] = value[r:r + 1, w * LANES:(w + 1) * LANES]
                    place += 1
        for copy in window_copies() + front_copies():
            copy.wait()
        for d, (k, off, cnt, width) in enumerate(FRONT):
            for t in range(cnt):
                front[d, pl.ds(t // width * 8 * width + t % width, 8, stride=width), :] = front_raw[d, t].astype(F32)
        window_send().start()
        for copy in front_sends():
            copy.start()

    def small_finish():
        total = front[me, pl.ds(0, TAIL), :]
        for o, copy in enumerate(front_sends()):
            copy.wait()
            total = total + front_land[o]
        window_send().wait()
        total = total * 0.125
        tail_g[...] = total

        @pl.when(me == 7)
        def _():
            n_out[...] += jnp.sum((total * total).reshape(TAIL // 8, 8, LANES), axis=0)
        copy = local(tail_g, g_flat.at[pl.ds(SEG_ROWS, TAIL)], l_tail)
        copy.start()
        copy.wait()

    def link_jobs(s):
        jobs = []
        for a in pair:
            half = jnp.where(s < BOTH, a, 1 - a)
            seg = jnp.where(s < HALF, diag, links[a])
            jobs.append((seg, (half * HALF + lax.rem(s, HALF)) * N, a * SLOTS + s))
        return jobs

    def own_jobs(j):
        return [(me, (h * HALF + j) * N, 2 * SLOTS + h * HALF + j) for h in pair]

    def raw_loads(jobs, kind, turn):
        for a, (seg, tile, slot) in enumerate(jobs):
            load_piece(refs, seg + turn, tile, raw.at[kind, a], l_raw.at[kind, a])

    def give(jobs, kind, par, wait_old, load=True):
        if load:
            raw_loads(jobs, kind, flip)
        for a, (seg, tile, slot) in enumerate(jobs):
            raw_wait(kind, a)
            copy = to_partner(par, a, slot)
            pl.when(wait_old)(copy.wait_send)

            def conv(d, a=a):
                stage_p[par, a, d] = raw[kind, a, d].astype(F32)
            tiles_loop(conv)
            copy.start()

    def step(s, count):
        j = lax.rem(s, HALF)
        ring = lax.rem(s, RING)

        @pl.when(s < SLOTS - 1)
        def _():
            give(link_jobs(s + 1), 0, lax.rem(s + 1, 2), s >= 1, False)
            pl.when(s < SLOTS - 2)(lambda: raw_loads(link_jobs(s + 2), 0, flip))

        @pl.when(s < SLOTS)
        def _():
            jobs = link_jobs(s)
            for a, (seg, tile, slot) in enumerate(jobs):
                to_partner(0, a, slot).wait_recv()
                local(land_p.at[slot], aux.at[0, a], l_aux.at[0, a]).start()

            @pl.when(s >= BOTH)
            def _():
                for a in pair:
                    to_link(0, a, j).wait_recv()
                for a in pair:
                    local(land_l.at[1 - a, j], aux.at[1, a], l_aux.at[1, a]).start()
            for a in pair:
                raw_wait(1, a)
                local(land_p.at[0], aux.at[0, a], l_aux.at[0, a]).wait()
                copy = to_link(ring, a, s)
                pl.when(s >= RING)(copy.wait_send)

                @pl.when(s < BOTH)
                def _(a=a):
                    def add(d):
                        stage[ring, a, d] = raw[1, a, d].astype(F32) + aux[0, a, d]
                    tiles_loop(add)

                @pl.when(s >= BOTH)
                def _(a=a):
                    local(land_p.at[0], aux.at[1, a], l_aux.at[1, a]).wait()

                    def add(d):
                        stage[ring, a, d] = raw[1, a, d].astype(F32) + aux[0, a, d] + aux[1, a, d]
                    tiles_loop(add)
                copy.start()
            pl.when(s < SLOTS - 1)(lambda: raw_loads(link_jobs(s + 1), 1, 0))

        pl.when(s == 2)(small_exchange)
        pl.when(s == BOTH + RING)(small_finish)

        @pl.when((s >= HALF + RING) & (s < BOTH + RING))
        def _():
            give(own_jobs(s - HALF - RING), 2, 2, s > HALF + RING)

        @pl.when(s >= BOTH + LAG)
        def _():
            take_own(s - BOTH - LAG)
        return count

    def take_own(j):
        for h, (seg, tile, slot) in enumerate(own_jobs(j)):
            load_piece(refs, seg, tile, raw.at[2, h], l_raw.at[2, h])
            to_partner(2, h, slot).wait_recv()
            local(land_p.at[slot], own_in.at[h, 0], l_own.at[h, 0]).start()
        for k in (1, 2):
            for h in pair:
                a = h if k == 1 else 1 - h
                slot = k * HALF + j
                to_link(0, a, slot).wait_recv()
                local(land_l.at[a, slot], own_in.at[h, k], l_own.at[h, k]).start()
        for h, (seg, tile, slot) in enumerate(own_jobs(j)):
            raw_wait(2, h)
            for a in trio:
                local(land_p.at[0], own_in.at[h, a], l_own.at[h, a]).wait()
            row = pl.multiple_of(tile * 8, 8)
            out = local(own_g.at[h], g_flat.at[pl.ds(row, ROWS)], l_g.at[h])
            pl.when(j >= 1)(out.wait)

            def relay(width, h=h):
                def body(r, acc):
                    for w in range(width):
                        t = r * width + w
                        g = (raw[2, h, t].astype(F32) + own_in[h, 0, t] + own_in[h, 1, t] + own_in[h, 2, t]) * 0.125
                        own_g[h, pl.ds(r * (8 * width) + w, 8, stride=width), :] = g
                        acc = acc + g * g
                    return acc
                n_out[...] += lax.fori_loop(0, N // width, body, jnp.zeros((8, LANES), F32))
            on_width(me, tile, relay)
            out.start()

    def state_loads(s):
        row, par = pl.multiple_of(s * ROWS, 8), lax.rem(s, 2)
        return [local(ins[a].at[pl.ds(row, ROWS)], st.at[par, a], l_in.at[par, a]) for a in trio]

    def gradient_load(s):
        row, par = pl.multiple_of(s * ROWS, 8), lax.rem(s, 2)
        return local(g_flat.at[pl.ds(row, ROWS + TAIL)], gb.at[par], l_in.at[par, 3])

    raw_loads(link_jobs(0), 0, flip)
    raw_loads(link_jobs(0), 1, 0)
    greet(others)
    give(link_jobs(0), 0, 0, False, False)
    raw_loads(link_jobs(1), 0, flip)
    lax.fori_loop(0, SLOTS + LAG, step, 0)
    for load in state_loads(0):
        load.start()
    gradient_load(0).start()

    norm_send[...] = n_out[...]
    norm_land[me] = n_out[...]

    def norm_copy(o, dev, slot):
        return remote(norm_send, norm_land.at[slot], s_n.at[o], r_n.at[slot], dev)
    for o, dev in enumerate(others):
        norm_copy(o, dev, me).start()
    for h in pair:
        local(own_g.at[h], g_flat.at[pl.ds(0, ROWS)], l_g.at[h]).wait()
    for o, dev in enumerate(others):
        norm_copy(o, dev, me).wait_send()
        norm_copy(o, dev, dev).wait_recv()
    n_out[...] = jnp.sum(norm_land[...], axis=0)
    norm = jnp.sqrt(jnp.sum(n_out[...], axis=(0, 1), keepdims=True))
    o_norm[...] = jnp.broadcast_to(norm, (8, LANES))
    n_out[...] = jnp.broadcast_to(jnp.minimum(1.0, MAX_NORM / (norm + CLIP_EPS)), (8, LANES))
    coef = n_out[pl.ds(0, 1), :]
    for a in pair:
        for par in trio:
            to_partner(par, a, 0).wait_send()
        for ring in range(RING):
            to_link(ring, a, 0).wait_send()

    def state_tail():
        copy = local(g_flat.at[pl.ds(WIN, 2 * TAIL)], window_g.at[pl.ds(0, 2 * TAIL)], l_tail)
        copy.start()
        copy.wait()
        place = lax.broadcasted_iota(jnp.int32, (56, LANES), 0) + (me * LOCAL_ROWS + WIN)
        decay = jnp.where(place < MATRIX_ROWS, WEIGHT_DECAY, 0.0)
        new = adam(window_g[pl.ds(shift, 56), :] * coef, window[0], window[1], window[2], lr, decay)
        gains_send[...] = new[0]
        for a in trio:
            window[a] = new[a]
            six_store(a).start()

        @pl.when(me == 7)
        def _():
            for o, dev in enumerate(others):
                gains_copy(o, dev).start()

    def six_store(a):
        return local(window.at[a, pl.ds(TAIL, 6)], outs[a].at[pl.ds(SEG_ROWS, 6)], l_six.at[a])

    def gains_copy(o, dev):
        return remote(gains_send, gains_land, s_gain.at[o], r_gain, dev)

    def gains_finish():
        def write(src):
            t = src[...]

            def row(r):
                return jnp.concatenate([t[6 + 9 * r + w:7 + 9 * r + w, :] for w in range(9)], axis=1)
            for out, rows in zip(gains_out, ((0, 1), (2, 3), (4,))):
                out[...] = jnp.concatenate([row(r) for r in rows], axis=0).astype(BF16)

        @pl.when(me == 7)
        def _():
            for o, dev in enumerate(others):
                gains_copy(o, dev).wait_send()
            write(gains_send)

        @pl.when(me != 7)
        def _():
            gains_copy(0, others[0]).wait_recv()
            write(gains_land)
        for a in trio:
            six_store(a).wait()

    def first_rows():
        part = pl.ds(54 - shift, TAIL)
        pb[pl.ds(0, TAIL), :] = adam(gb[0, pl.ds(0, TAIL), :] * coef, *[halo[a, part, :] for a in trio], lr, WEIGHT_DECAY)[0]

    def at(seg, c):
        return land.at[seg, pl.ds(pl.multiple_of(c * N, N), N)]

    def place(a, seg, chunk, q, act):
        low = (1 + a) * HALF - LATE
        late = (q >= low) & (q < low + LATE)
        pl.when(late)(lambda: act(spare[a].at[pl.ds((q - low) * N, N)]))
        pl.when(jnp.logical_not(late))(lambda: act(at(seg, chunk)))

    def link_piece(q, a):
        direct = q < BOTH
        return jnp.where(direct, links[a], diag), jnp.where(direct, q, q - (1 + a) * HALF)

    def own(s):
        ring = lax.rem(s, RING)
        row = pl.multiple_of(s * ROWS, 8)

        par = lax.rem(s, 2)

        def state_store(a, par):
            return local(st.at[par, a], outs[a].at[pl.ds(row, ROWS)], l_out.at[par, a])

        @pl.when(s < BOTH - 1)
        def _():
            gradient_load(s + 1).start()
            for a, load in enumerate(state_loads(s + 1)):
                pl.when(s >= 1)(state_store(a, 1 - par).wait)
                load.start()
        for load in state_loads(s) + [gradient_load(s)]:
            load.wait()
        pl.when(s == 0)(first_rows)
        slab = 48
        base = me * LOCAL_ROWS + s * ROWS

        def update(i, carry):
            d = pl.ds(pl.multiple_of(i * slab, 8), slab)
            e = pl.ds(i * slab + shift, slab)
            rows = lax.broadcasted_iota(jnp.int32, (slab, LANES), 0) + (base + i * slab)
            decay = jnp.where(rows < MATRIX_ROWS, WEIGHT_DECAY, 0.0)
            new = adam(gb[par, e, :] * coef, *[st[par, a, d, :] for a in trio], lr, decay)
            for a in trio:
                st[par, a, d, :] = new[a]
            pb[e, :] = new[0]
            return carry
        lax.fori_loop(0, ROWS // slab, update, 0)
        for a in trio:
            state_store(a, par).start()
        devs = links + (partner,)

        @pl.when(s >= RING)
        def _():
            for a in trio:
                remote(stage_u.at[ring], at(me, s), su.at[a, ring], ru_o.at[s], devs[a]).wait_send()

        def relay(width):
            def body(r, carry):
                for w in range(width):
                    stage_u[ring, r * width + w] = pb[pl.ds(r * (8 * width) + w, 8, stride=width), :]
                return carry
            lax.fori_loop(0, N // width, body, 0)
        on_width(me, s * N, relay)
        pb[pl.ds(0, TAIL), :] = pb[pl.ds(ROWS, TAIL), :]
        for a in pair:
            place(a, me, s, s, lambda ref, a=a: remote(stage_u.at[ring], ref, su.at[a, ring], ru.at[a, s], devs[a]).start())
        remote(stage_u.at[ring], at(me, s), su.at[2, ring], ru_o.at[s], partner).start()

        def conv(d):
            cout[5, d] = stage_u[ring, d].astype(BF16)
        tiles_loop(conv)
        store_piece(outs7, me, s * N, cout.at[5], l_so.at[5])

    def convert(k, seg, chunk):
        local(at(0, 0), cin.at[k], l_c.at[k]).wait()

        def conv(d):
            cout[k, d] = cin[k, d].astype(BF16)
        tiles_loop(conv)
        store_piece(outs7, seg, chunk * N, cout.at[k], l_so.at[k])

    def fetch(k, ref):
        local(ref, cin.at[k], l_c.at[k]).start()

    def stored(k):
        local(cout.at[k], outs7[0].at[pl.ds(0, N)], l_so.at[k]).wait()

    last = SLOTS - LATE - 1
    spot = at(0, 0)

    def link_wait(a, q):
        return remote(spot, spot, s_d.at[a, 0], ru.at[a, q], links[a])

    def hand(a, par, q, src, dst):
        return remote(src, dst, s_d.at[a, par], r_d.at[a, q], partner)

    def forward(a, seg, chunk, j, dst):
        return remote(at(seg, chunk), dst, s_f.at[a, j], ru.at[a, BOTH + j], links[a])

    def start_forward(a, seg, chunk, j):
        pl.when(j < HALF - LATE - 1)(lambda: forward(a, seg, chunk, j, at(seg, chunk)).start())
        pl.when(j == HALF - LATE - 1)(lambda: forward(a, seg, chunk, j, ends[a]).start())

    def gather_step(s, carry):
        j = s - BOTH
        q = s - LAG
        z = q - 1
        par = lax.rem(s, 2)
        arrives = (q >= 0) & (q < last)
        from_partner = (z >= 0) & (z < last)
        own_partner = (z >= 0) & (z < BOTH)
        pl.when(s == 2)(state_tail)
        pl.when((s >= 1) & (s <= BOTH))(lambda: stored(5))
        pl.when(s < BOTH)(lambda: own(s))

        @pl.when((j >= 0) & (j < HALF - LATE))
        def _():
            start_forward(1, xn, j, j)
            start_forward(0, yn, HALF + j, j)

        @pl.when((q >= 1) & (q <= last))
        def _():
            for a in pair:
                stored(a)

        @pl.when((z >= 1) & (z <= last))
        def _():
            for a in pair:
                stored(2 + a)

        pl.when((z >= 1) & (z <= BOTH))(lambda: stored(4))

        @pl.when(arrives)
        def _():
            for a in pair:
                seg, chunk = link_piece(q, a)
                link_wait(a, q).wait_recv()
                pl.when(q >= 2)(hand(a, par, q, spot, spot).wait_send)

                def act(ref, a=a, seg=seg, chunk=chunk):
                    hand(a, par, q, ref, at(seg, chunk)).start()
                    fetch(a, ref)
                place(a, seg, chunk, q, act)

        @pl.when(own_partner)
        def _():
            remote(spot, spot, su.at[2, 0], ru_o.at[z], partner).wait_recv()
            fetch(4, at(partner, z))

        @pl.when(from_partner)
        def _():
            for a in pair:
                seg, chunk = link_piece(z, a)
                hand(a, 0, z, spot, spot).wait_recv()
                fetch(2 + a, at(seg + flip, chunk))

        @pl.when(arrives)
        def _():
            for a in pair:
                convert(a, *link_piece(q, a))

        pl.when(own_partner)(lambda: convert(4, partner, z))

        @pl.when(from_partner)
        def _():
            for a in pair:
                seg, chunk = link_piece(z, a)
                convert(2 + a, seg + flip, chunk)
        return carry

    lax.fori_loop(0, last + LAG + 1, gather_step, 0)
    gains_finish()
    for a in pair:
        link_wait(a, last).wait_recv()
    for a in pair:
        stored(2 + a)
        for par in pair:
            hand(a, par, 0, spot, spot).wait_send()
        for j in range(HALF - LATE):
            forward(a, 0, 0, j, spot).wait_send()
    for a in trio:
        for par in pair:
            local(st.at[par, a], outs[a].at[pl.ds(0, ROWS)], l_out.at[par, a]).wait()
        for ring in range(RING):
            remote(stage_u.at[ring], at(me, 0), su.at[a, ring], ru_o.at[0], partner).wait_send()


def copy_kernel(*args):
    ins, outs, (wide, thin, l_in, l_out) = args[:10], args[10:20], args[20:]
    depth = wide.shape[0]
    jobs = []
    for src, dst in zip(ins, outs):
        size, kind = src.shape[0], len(src.shape) - 2
        piece = (SEG_ROWS // 8, COUNTS[1])[kind]
        for off in range(0, size, piece):
            rows = pl.ds(off, min(piece, size - off))
            n = len(jobs)
            buf = (wide, thin)[kind].at[n % depth, pl.ds(0, rows.size)]
            jobs.append((local(src.at[rows], buf, l_in.at[n % depth]), local(buf, dst.at[rows], l_out.at[n % depth])))
    ahead = depth // 2
    for n in range(len(jobs) + ahead):
        if n < len(jobs):
            if n >= depth:
                jobs[n - depth][1].wait()
            jobs[n][0].start()
        if n >= ahead:
            jobs[n - ahead][0].wait()
            jobs[n - ahead][1].start()
    for job in jobs[-depth:]:
        job[1].wait()


def late_kernel(mine, *args):
    came, ends, outs7 = args[:2], args[2:4], args[11:18]
    cin, cout, l_in, l_out = args[18:]
    flip, partner, xn, yn, diag = neighbours(lax.axis_index("dp"))
    seg = diag if mine else diag + flip
    jobs = [(a, i, a * (LATE + 1) + i) for a in range(2) for i in range(LATE + 1)]
    loads = [local(came[a].at[pl.ds(i * N, N)] if i < LATE else ends[a], cin.at[k], l_in.at[k]) for a, i, k in jobs]
    for load in loads:
        load.start()
    for a, i, k in jobs:
        loads[k].wait()

        def conv(d, k=k):
            cout[k, d] = cin[k, d].astype(BF16)
        tiles_loop(conv)
        chunk = (1 + a) * HALF - LATE + (i if i < LATE else -1)
        store_piece(outs7, seg, chunk * N + 0 * seg, cout.at[k], l_out.at[k])
    for a, i, k in jobs:
        local(cout.at[k], outs7[0].at[pl.ds(0, N)], l_out.at[k]).wait()


ANY = pl.BlockSpec(memory_space=pl.ANY)
VMEM = pl.BlockSpec(memory_space=pltpu.VMEM)
SMEM = pl.BlockSpec(memory_space=pltpu.SMEM)


def to_tiles(x):
    cols = x.shape[-1]
    lead = x.size // cols
    return x.reshape(lead // 8, 8, cols // LANES, LANES).transpose(0, 2, 1, 3).reshape(-1, 8, LANES)


def from_tiles(t, shape):
    cols = shape[-1]
    lead = t.size // cols
    return t.reshape(lead // 8, cols // LANES, 8, LANES).transpose(0, 2, 1, 3).reshape(shape)


def shapes(kind, dtype, *dims):
    return [kind(d, dtype) for d in dims]


def dmas(*dims):
    return [pltpu.SemaphoreType.DMA(d) if d else pltpu.SemaphoreType.DMA for d in dims]


def params_of(**kw):
    return pltpu.CompilerParams(vmem_limit_bytes=LIMIT, has_side_effects=True, **kw)


def copy_call(arrays):
    depth = 12
    moved = 2 * sum(a.size * a.dtype.itemsize for a in arrays)
    return pl.pallas_call(
        copy_kernel,
        out_shape=[jax.ShapeDtypeStruct(a.shape, a.dtype) for a in arrays],
        in_specs=[ANY] * 10,
        out_specs=[ANY] * 10,
        scratch_shapes=[pltpu.VMEM((depth, SEG_ROWS // 8, LANES), F32), pltpu.VMEM((depth, COUNTS[1], 8, LANES), BF16)] + dmas((depth,), (depth,)),
        compiler_params=params_of(),
        cost_estimate=pl.CostEstimate(flops=100 * moved, bytes_accessed=moved, transcendentals=0),
        name="copy_results",
    )(*arrays)


def late_call(mine, came, tiles):
    chunks = 2 * LATE + 2
    return pl.pallas_call(
        functools.partial(late_kernel, mine),
        out_shape=[jax.ShapeDtypeStruct(a.shape, a.dtype) for a in tiles],
        in_specs=[ANY] * 11,
        out_specs=[ANY] * 7,
        input_output_aliases={4 + k: k for k in range(7)},
        scratch_shapes=[pltpu.VMEM((chunks, N, 8, LANES), F32), pltpu.VMEM((chunks, N, 8, LANES), BF16)] + dmas((chunks,), (chunks,)),
        compiler_params=params_of(),
        cost_estimate=pl.CostEstimate(flops=came[0].size * 1000, bytes_accessed=came[0].size * 12, transcendentals=0),
        name="late_chunks",
    )(*came, *tiles)


def local_step(*arrays):
    grads = arrays[:10]
    states = [a.reshape(LOCAL_ROWS, LANES) for a in arrays[10:13]]
    chunk = (N, 8, LANES)
    sds = jax.ShapeDtypeStruct
    vm = pltpu.VMEM
    deep = len(FRONT)
    late = (LATE * N, 8, LANES)
    two, three, eight, width = 2, 3, 8, 1152
    tile, tail, long = (eight, LANES), (56, LANES), (104, LANES)
    res = pl.pallas_call(
        step_kernel,
        out_shape=shapes(sds, F32, *[(LOCAL_ROWS, LANES)] * three) + shapes(sds, BF16, *[(c, eight, LANES) for c in COUNTS], (two, width), (two, width), (1, width))
        + shapes(sds, F32, (eight, LANES), (SEG_ROWS + TAIL, LANES), (two, SLOTS) + chunk, (2 * SLOTS + BOTH,) + chunk, (eight, SEG_TILES, eight, LANES), late, late, chunk, chunk),
        in_specs=[ANY] * 7 + [VMEM] * 3 + [ANY] * 3 + [SMEM],
        out_specs=[ANY] * 10 + [VMEM] * 4 + [ANY] * 8,
        scratch_shapes=shapes(vm, BF16, (three, two) + chunk)
        + shapes(vm, F32, (three, two) + chunk, (RING,) + chunk, (two, two) + chunk, (RING, two) + chunk, (two, three) + chunk, (two, ROWS, LANES),
                 tile, (eight, *tile), tile)
        + shapes(vm, BF16, (deep, 24, eight, LANES))
        + shapes(vm, F32, (eight, 192, LANES), (deep, TAIL, LANES), (TAIL, LANES), (three, *tail), (three, *long), long, tail, tail,
                 (two, ROWS + TAIL, LANES), (two, three, ROWS, LANES), (ROWS + TAIL, LANES), (5,) + chunk)
        + shapes(vm, BF16, (6,) + chunk)
        + dmas((RING, two), (three, two), (two, SLOTS), (2 * SLOTS + BOTH,), (three, two), (two, two), (two, three), (two,), (deep,), (eight,),
               (deep,), (deep,), (deep,), (6,), None, None, None, (three,), (deep,), None,
               (three, RING), (two, SLOTS), (BOTH,), (two, SLOTS), (two, HALF), (two, two), (two, 4), (two, three), (5,), (6,)),
        compiler_params=params_of(collective_id=0),
        name="adamw_step",
    )(*[to_tiles(x) for x in grads[:7]], *grads[7:], *states, arrays[13].reshape(1))
    kept, (norm, spare_x, spare_y) = res[:10], (res[13], *res[18:20])

    def swap(x, bit):
        return lax.ppermute(x, "dp", [(i, i ^ bit) for i in range(8)])
    ends = res[:-3:-1]
    came = [swap(spare_x, 4), swap(spare_y, 2)] + [swap(e, 1) for e in ends]
    copied = list(copy_call(kept))
    *came, copied[4] = lax.optimization_barrier((*came, copied[4]))
    tiles = late_call(True, (*came[:2], *ends), copied[3:])
    tiles = late_call(False, (*[swap(c, 1) for c in came[:2]], *came[2:]), tiles)
    params = [from_tiles(t, x.shape[1:]) for t, x in zip(tiles, grads[:7])]
    return tuple([a.reshape(-1) for a in copied[:3]] + params + [res[10], res[11], res[12].reshape(-1), norm[0, 0]])


def solution(mesh):
    return jax.shard_map(local_step, mesh=mesh, in_specs=(P("dp"),) * 13 + (P(),), out_specs=(P("dp"),) * 3 + (P(),) * 11, check_vma=False)
```
